128 devices in a mesh: pipe: 2 (over x_lo), tensor: 4 (over x_hi, core), dp: 16 (over z, y).
Axes of the slice: x: 4 (x_hi: 2, x_lo: 2; x = x_hi * 2 + x_lo), y: 4, z: 4, core: 2. Of those that a mesh axis runs over, the one named last changes fastest.
Arguments:
- inputs: bfloat16 [2, 2048, 16384], P(None, 'dp', 'tensor'), may hold values from -6 to 6
- w_in: bfloat16 [2, 16384, 1024], P('pipe', ('tensor', 'dp')), may hold values from -0.046875 to 0.046875
- w_out: bfloat16 [2, 1024, 16384], P('pipe', None, ('tensor', 'dp')), may hold values from -0.1875 to 0.1875
- cotangent: bfloat16 [2, 2048, 16384], P(None, 'dp', 'tensor'), may hold values from -6 to 6
Outputs:
- update_in: float32 [2, 16384, 1024], P('pipe', ('tensor', 'dp'))
- update_out: float32 [2, 1024, 16384], P('pipe', None, ('tensor', 'dp'))
- grad_norm: float32 [], replicated
The draws below stay inside these ranges and needn't reach their ends.
All inputs are finite; a program needn't handle non-finite values.
Results may differ from the reference program's by a relative error of at most 0.008.
Values may be sent and summed in bfloat16 or wider, within the bound.
No kernel may reach another device: no remote copies, remote signals or barrier semaphores. Data moves between devices by JAX's collectives and lax.ppermute only.
A program may use at most 192 MiB of HBM per device.

```python
import jax
import jax.numpy as jnp
from jax import lax

D = 16384
H = 1024
MB = 2
TOK = 128
SECTIONS = 2
BATCH = 2048
CLIP_NORM = 16384


def steps_of(key, dims, cuts, low, high):
    def one(dim, shards_of):
        draws = jax.random.uniform(jax.random.fold_in(jax.random.fold_in(key, 6), dim), (shards_of,), jnp.float32, low / len(cuts), high / len(cuts))
        return jnp.repeat(jnp.exp(draws), dims[dim] // shards_of).reshape((-1,) + (1,) * (len(dims) - dim - 1))

    gain = one(*cuts[0])
    for cut in cuts[1:]:
        gain = gain * one(*cut)
    return gain


def gaussian(key, extent, scale, most, split=(), dtype=jnp.bfloat16):
    gain = steps_of(key, extent, split, -0.22, 0.18) if split else 1.0
    values = jax.random.normal(key, extent, jnp.float32) * scale * gain
    return jnp.minimum(jnp.maximum(values, -most), most).astype(dtype)


def setup_inputs(seed: int = 0) -> dict:
    keys = jax.random.split(jax.random.key(seed), 5)
    return {
        "inputs": gaussian(keys[0], (MB, BATCH, D), 1.0, 6.0, ((1, 16), (2, 4))),
        "w_in": gaussian(keys[1], (SECTIONS, D, H), D ** -0.5, 0.046875, ((0, 2), (1, 64))),
        "w_out": gaussian(keys[2], (SECTIONS, H, D), H ** -0.5, 0.1875, ((0, 2), (2, 64))),
        "cotangent": gaussian(keys[3], (MB, BATCH, D), 1.0, 6.0, ((1, 16), (2, 4))),
    }


def silu_round(preact):
    return jax.nn.silu(preact).astype(jnp.bfloat16)

def slope_round(upward, preact):
    sigmoid_value = jax.nn.sigmoid(preact)
    return (upward * sigmoid_value * (1.0 + preact * (1.0 - sigmoid_value))).astype(jnp.bfloat16)

def kahan_add(running, carried, grad_term):
    corrected = grad_term - carried.astype(jnp.float32)
    summed = (running.astype(jnp.float32) + corrected).astype(jnp.bfloat16)
    carried = (summed.astype(jnp.float32) - running.astype(jnp.float32) - corrected).astype(jnp.bfloat16)
    return (summed, carried)

def reference(inputs, w_in, w_out, cotangent):
    replicas = BATCH // TOK
    stored_x = []
    stored_pre = []
    stored_act = []
    for micro_index in range(MB):
        current = inputs[micro_index]
        list_x, list_pre, list_act = ([], [], [])
        for layer in range(SECTIONS):
            preact = jnp.dot(current, w_in[layer], preferred_element_type=jnp.float32)
            activation = silu_round(preact)
            list_x.append(current)
            list_pre.append(preact)
            list_act.append(activation)
            current = (current.astype(jnp.float32) + jnp.dot(activation, w_out[layer], preferred_element_type=jnp.float32)).astype(jnp.bfloat16)
        stored_x.append(list_x)
        stored_pre.append(list_pre)
        stored_act.append(list_act)
    errors = [cotangent[micro_index] for micro_index in range(MB)]
    totals_in = [None] * SECTIONS
    totals_out = [None] * SECTIONS
    for layer in reversed(range(SECTIONS)):
        sum_in = jnp.zeros((replicas, D, H), jnp.bfloat16)
        err_in = jnp.zeros((replicas, D, H), jnp.bfloat16)
        sum_out = jnp.zeros((replicas, H, D), jnp.bfloat16)
        err_out = jnp.zeros((replicas, H, D), jnp.bfloat16)
        for micro_index in range(MB):
            upper = errors[micro_index]
            upward = jnp.dot(upper, w_out[layer].T, preferred_element_type=jnp.float32)
            slope = slope_round(upward, stored_pre[micro_index][layer])
            x_groups = stored_x[micro_index][layer].reshape(replicas, TOK, D).astype(jnp.float32)
            slope_groups = slope.reshape(replicas, TOK, H).astype(jnp.float32)
            act_groups = stored_act[micro_index][layer].reshape(replicas, TOK, H).astype(jnp.float32)
            err_groups = upper.reshape(replicas, TOK, D).astype(jnp.float32)
            grad_in = jnp.einsum('gtc,gth->gch', x_groups, slope_groups)
            grad_out = jnp.einsum('gth,gtc->ghc', act_groups, err_groups)
            sum_in, err_in = kahan_add(sum_in, err_in, grad_in)
            sum_out, err_out = kahan_add(sum_out, err_out, grad_out)
            errors[micro_index] = (upper.astype(jnp.float32) + jnp.dot(slope, w_in[layer].T, preferred_element_type=jnp.float32)).astype(jnp.bfloat16)
        totals_in[layer] = lax.optimization_barrier(jnp.sum(sum_in.astype(jnp.float32) - err_in.astype(jnp.float32), axis=0))
        totals_out[layer] = lax.optimization_barrier(jnp.sum(sum_out.astype(jnp.float32) - err_out.astype(jnp.float32), axis=0))
    total_in = jnp.stack(totals_in)
    total_out = jnp.stack(totals_out)
    grad_norm = jnp.sqrt(jnp.sum(total_in * total_in) + jnp.sum(total_out * total_out))
    factor = jnp.minimum(1.0, CLIP_NORM / grad_norm)
    return (total_in * factor, total_out * factor, grad_norm)
```

```python
import jax
import jax.numpy as jnp
from jax import lax
from jax.sharding import Mesh
from jax.sharding import PartitionSpec as P

CLIP_NORM = 16384
AXES = ("p", "h", "c", "z", "y")
BF = jnp.bfloat16
F32 = jnp.float32


def dot(a, b):
    return jnp.dot(a, b, preferred_element_type=F32)


def dot_t0(a, b):
    return lax.dot_general(a, b, (((0,), (0,)), ((), ())), preferred_element_type=F32)


def dot_t1(a, b):
    return lax.dot_general(a, b, (((1,), (1,)), ((), ())), preferred_element_type=F32)


def a2a(value, axes):
    return lax.all_to_all(value, axes, 0, 0, tiled=True)


def silu_bf(pre):
    return jax.nn.silu(pre).astype(BF)


def slope_bf(up, pre):
    s = jax.nn.sigmoid(pre)
    return (up * s * (1.0 + pre * (1.0 - s))).astype(BF)


def on_device(inputs, w_in, w_out, cotangent):
    first = lax.axis_index("p") == 0
    z_index = lax.axis_index("z")
    n_micro, rows, cols = inputs.shape
    tok = n_micro * rows
    hidden = w_in.shape[2]
    own = w_in.shape[1]
    nz, ny, nc = lax.axis_size("z"), lax.axis_size("y"), lax.axis_size("c")
    n_ph = lax.axis_size("p") * lax.axis_size("h")
    half = tok // nc
    mine = half // n_ph
    wide = own * nz

    w_i = w_in[0]
    w_o = w_out[0].T
    w_u = jnp.where(first, w_o, w_i)
    w_v = jnp.where(first, w_i, w_o)
    w_3 = lax.ppermute(w_u, "p", [(0, 1), (1, 0)])
    w_u = lax.all_gather(w_u, "z", axis=0, tiled=True)
    w_v = lax.all_gather(w_v, "y", axis=0, tiled=True)
    w_3 = lax.all_gather(w_3, "z", axis=0, tiled=True)

    x = inputs.reshape(tok, nz, ny, own)
    ct = cotangent.reshape(tok, nz, ny, own)
    u = jnp.where(first, ct, x).transpose(2, 0, 1, 3).reshape(ny * tok, wide)
    v = jnp.where(first, x, ct).transpose(1, 0, 2, 3).reshape(nz * tok, ny * own)
    u = a2a(u, "y")
    v = a2a(v, "z")

    left = jnp.where(first, w_u, w_3)
    right = jnp.where(first, w_3, w_u)
    block = hidden // nz
    left = lax.dynamic_slice_in_dim(left, z_index * block, block, 1)
    m_part = a2a(dot_t0(left, right).astype(BF), ("y", "h", "c"))
    m_rows = m_part.reshape(-1, block // (ny * 4), hidden).astype(F32).sum(0).astype(BF)
    m_rows = lax.all_gather(m_rows, ("h", "c"), axis=0, tiled=True)
    m_all = lax.all_gather(m_rows, ("z", "y"), axis=0, tiled=True)

    a_u = dot(u, w_u).astype(BF).reshape(ny, nc, half, hidden).transpose(1, 0, 2, 3)
    a_v = dot(v, w_v).astype(BF).reshape(nz, nc, half, hidden).transpose(1, 0, 2, 3)
    a_u, a_v = a2a(a_u, "c"), a2a(a_v, "c")
    a_u = a_u.astype(F32).sum(0).astype(BF)
    a_v = a_v.astype(F32).sum(0).astype(BF)
    a_u, a_v = a2a(a_u, "y"), a2a(a_v, "z")
    a_u = a_u.astype(F32).sum(0).astype(BF).reshape(n_ph, mine, hidden)
    a_v = a_v.astype(F32).sum(0).astype(BF).reshape(n_ph, mine, hidden)
    both = a2a(jnp.concatenate([a_u, a_v], 2), ("p", "h"))
    both = both.reshape(2, n_ph // 2, mine, 2 * hidden).astype(F32).sum(1)

    pre0, up0 = both[0, :, hidden:], both[0, :, :hidden]
    pre1, up1 = both[1, :, :hidden], both[1, :, hidden:]
    act0 = silu_bf(pre0)
    pre1 = pre1 + dot(act0, m_all)
    act1 = silu_bf(pre1)
    slope1 = slope_bf(up1, pre1)
    up0 = up0 + dot_t1(slope1, m_all)
    slope0 = slope_bf(up0, pre0)

    to_first = jnp.stack([slope0, act0, slope1])
    to_last = jnp.stack([act1, slope1, act0])
    out = jnp.stack([to_first] * (n_ph // 2) + [to_last] * (n_ph // 2))
    out = a2a(out, ("p", "h")).transpose(1, 0, 2, 3).reshape(3, half, hidden)
    r = lax.all_gather(out[:1], "z", axis=1)
    pq = lax.all_gather(out[1:], "y", axis=1)
    rpq = jnp.concatenate([r, pq], 0)
    rpq = lax.all_gather(rpq, "c", axis=2).reshape(3, nz * tok, hidden)
    r, p, q = rpq[0], rpq[1], rpq[2]

    g_v = dot_t0(v, r).astype(BF)
    g_v = lax.psum_scatter(g_v, "y", scatter_dimension=0, tiled=True).astype(F32)
    u = (u.astype(F32) + dot_t1(q, w_3)).astype(BF)
    g_u = a2a(dot_t0(u, p).astype(BF), "z")
    g_u = g_u.reshape(nz, own, hidden).astype(F32).sum(0)

    squares = jnp.sum(g_u * g_u) + jnp.sum(g_v * g_v)
    grad_norm = jnp.sqrt(lax.psum(squares, AXES))
    factor = jnp.minimum(1.0, CLIP_NORM / grad_norm)
    g_in = jnp.where(first, g_v, g_u) * factor
    g_out = jnp.where(first, g_u, g_v) * factor
    return (g_in[None], g_out.T[None], grad_norm)


def solution(mesh):
    split = Mesh(mesh.devices.reshape(mesh.shape["pipe"], 2, 2, 4, 4), AXES)
    tensor, dp, all_model = ("h", "c"), ("z", "y"), ("h", "c", "z", "y")
    placed = (
        P(None, dp, tensor),
        P("p", all_model, None),
        P("p", None, all_model),
        P(None, dp, tensor),
    )
    return jax.shard_map(
        on_device,
        mesh=split,
        in_specs=placed,
        out_specs=(P("p", all_model, None), P("p", None, all_model), P()),
        check_vma=False,
    )
```

```python
import functools

import jax
import jax.numpy as jnp
from jax import lax
from jax.experimental import pallas as pl
from jax.experimental.pallas import tpu as pltpu
from jax.sharding import Mesh
from jax.sharding import PartitionSpec as P

CLIP_NORM = 16384
AXES = ("p", "h", "c", "z", "y")
BF = jnp.bfloat16
F32 = jnp.float32


def dot(a, b):
    return jnp.dot(a, b, preferred_element_type=F32)


def dot_t0(a, b):
    return lax.dot_general(a, b, (((0,), (0,)), ((), ())), preferred_element_type=F32)


def dot_t1(a, b):
    return lax.dot_general(a, b, (((1,), (1,)), ((), ())), preferred_element_type=F32)


def a2a(value, axes):
    return lax.all_to_all(value, axes, 0, 0, tiled=True)


def shift(value, axis, by):
    count = lax.axis_size(axis)
    return lax.ppermute(value, axis, [(i, (i + by) % count) for i in range(count)])


def shift_x(value, by):
    pairs = []
    for p in range(2):
        for h in range(2):
            to = (h * 2 + p + by) % 4
            pairs.append((p * 2 + h, (to % 2) * 2 + to // 2))
    return lax.ppermute(value, ("p", "h"), pairs)


def silu_bf(pre):
    return jax.nn.silu(pre).astype(BF)


def slope_bf(up, pre):
    s = jax.nn.sigmoid(pre)
    return (up * s * (1.0 + pre * (1.0 - s))).astype(BF)


def cut_kernel(along_z, at_ref, one_ref, two_ref, *outs):
    p, x, c, z, y = (at_ref[i] for i in range(5))
    tok = one_ref.shape[0]
    own = one_ref.shape[1] // 16
    half, part = tok // 2, tok // 8
    for rc in range(2):
        for q in range(4):
            source = lax.rem(c + rc, 2) * half + lax.rem(x + 4 - q, 4) * part
            rows = pl.ds(pl.multiple_of(source, part), part)
            to = rc * half + q * part
            for k in range(4):
                for j in range(4):
                    if along_z:
                        zz, yy = lax.rem(z + k, 4), lax.rem(y + 4 - j, 4)
                    else:
                        zz, yy = lax.rem(z + 4 - j, 4), lax.rem(y + k, 4)
                    cols = pl.ds(pl.multiple_of((zz * 4 + yy) * own, own), own)
                    got = jnp.where(p == 0, one_ref[rows, cols], two_ref[rows, cols])
                    outs[k][to : to + part, j * own : (j + 1) * own] = got


def cut(at, one, two, along_z):
    tok, width = one.shape
    vmem = pl.BlockSpec(memory_space=pltpu.VMEM)
    return pl.pallas_call(
        functools.partial(cut_kernel, along_z),
        out_shape=[jax.ShapeDtypeStruct((tok, width // 4), BF)] * 4,
        in_specs=[pl.BlockSpec(memory_space=pltpu.SMEM), vmem, vmem],
        out_specs=[vmem] * 4,
        name="cut_z" if along_z else "cut_y",
    )(at, one, two)


def gather(value, axis):
    return [value] + [shift(value, axis, k) for k in (1, 2, 3)]


def exchange(pieces, axis, sign):
    return [pieces[0]] + [shift(pieces[k], axis, sign * k) for k in (1, 2, 3)]


def sum_back(blocks, axis):
    parts = exchange([blocks[0]] + [b.astype(BF) for b in blocks[1:]], axis, -1)
    return sum((part.astype(F32) for part in parts[1:]), parts[0])


def on_device(inputs, w_in, w_out, cotangent):
    p, h, c, z, y = (lax.axis_index(a) for a in AXES)
    first = p == 0
    n_micro, rows, cols = inputs.shape
    tok = n_micro * rows
    hidden = w_in.shape[2]
    own = w_in.shape[1]
    half = tok // 2
    mine = half // 4

    w_i = w_in[0]
    w_o = w_out[0].T
    w_u = jnp.where(first, w_o, w_i)
    w_v = jnp.where(first, w_i, w_o)
    w_3 = lax.ppermute(w_u, "p", [(0, 1), (1, 0)])
    w_vs = gather(w_v, "y")
    w_us = gather(w_u, "z")

    at = jnp.stack([p, h * 2 + p, c, z, y])
    x = inputs.reshape(tok, cols)
    ct = cotangent.reshape(tok, cols)
    v_blocks = exchange(cut(at, x, ct, True), "z", 1)
    u_blocks = exchange(cut(at, ct, x, False), "y", 1)

    left = jnp.where(first, w_u, w_3)
    right = jnp.where(first, w_3, w_u)
    left = left.reshape(own, 16, 2, hidden // 32)
    left = lax.dynamic_index_in_dim(left, p, 2, False).reshape(own, hidden // 2)
    m_part = a2a(dot_t0(left, right).astype(BF), ("z", "y", "h", "c"))
    m_rows = m_part.reshape(64, hidden // 128, hidden).astype(F32).sum(0).astype(BF)
    m_rows = jnp.broadcast_to(m_rows[None], (8,) + m_rows.shape)
    m_rows = a2a(m_rows, ("p", "h", "c")).reshape(hidden // 16, hidden)
    m_all = lax.all_gather(m_rows, ("z", "y"), axis=0, tiled=True)

    def split_rows(blocks):
        return jnp.concatenate([b[:half] for b in blocks] + [b[half:] for b in blocks])

    def reduced(blocks, w_all, axis):
        sent = shift(dot(blocks[4 * half :], w_all).astype(BF), "c", 1)
        kept = dot(blocks[: 4 * half], w_all) + sent.astype(F32)
        return sum_back([kept[k * half : (k + 1) * half] for k in range(4)], axis)

    v = split_rows(v_blocks)
    u = split_rows(u_blocks)
    a_v = reduced(v, jnp.concatenate(w_vs), "z")
    a_u = reduced(u, jnp.concatenate(w_us), "y")
    a_u, a_v, w_3 = lax.optimization_barrier((a_u, a_v, w_3))
    w_3 = jnp.concatenate(gather(w_3, "z"))

    both = jnp.concatenate([a_u, a_v], 1)
    pieces = [both[(4 - k) % 4 * mine :][:mine] for k in range(4)]
    got = [pieces[0]] + [shift_x(pieces[k].astype(BF), k).astype(F32) for k in (1, 2, 3)]
    same = got[0] + got[2]
    other = got[1] + got[3]
    layer0 = jnp.where(first, same, other)
    layer1 = jnp.where(first, other, same)
    up0, pre0 = layer0[:, :hidden], layer0[:, hidden:]
    pre1, up1 = layer1[:, :hidden], layer1[:, hidden:]
    act0 = silu_bf(pre0)
    pre1 = pre1 + dot(act0, m_all)
    act1 = silu_bf(pre1)
    slope1 = slope_bf(up1, pre1)
    up0 = up0 + dot_t1(slope1, m_all)
    slope0 = slope_bf(up0, pre0)

    to_first = jnp.stack([slope0, act0, slope1])
    to_last = jnp.stack([act1, slope1, act0])
    same = jnp.where(first, to_first, to_last)
    other = jnp.where(first, to_last, to_first)
    got = [same, shift_x(other, 1), shift_x(same, 2), shift_x(other, 3)]
    rpq = jnp.concatenate(got, 1)
    r = jnp.concatenate(gather(rpq[0], "z"))
    pq = jnp.concatenate(gather(rpq[1:], "y"), 1)
    far_r, far_pq = shift(r, "c", 1), shift(pq, "c", 1)
    r = jnp.concatenate([r, far_r])
    pq = jnp.concatenate([pq, far_pq], 1)

    g_v = dot_t0(v, r)
    g_v = sum_back([g_v[k * own : (k + 1) * own] for k in range(4)], "y")
    u = (u.astype(F32) + dot_t1(pq[1], w_3)).astype(BF)
    g_u = dot_t0(u, pq[0])
    g_u = sum_back([g_u[k * own : (k + 1) * own] for k in range(4)], "z")

    squares = jnp.sum(g_u * g_u) + jnp.sum(g_v * g_v)
    for axes, count in ((("z", "y"), 16), (("p", "h", "c"), 8)):
        row = jnp.broadcast_to(squares, (count, 8, 128))
        squares = a2a(row, axes)[:, 0, 0].sum()
    grad_norm = jnp.sqrt(squares)
    factor = jnp.minimum(1.0, CLIP_NORM / grad_norm)
    g_in = jnp.where(first, g_v, g_u) * factor
    g_out = jnp.where(first, g_u, g_v) * factor
    return (g_in[None], g_out.T[None], grad_norm)


def solution(mesh):
    split = Mesh(mesh.devices.reshape(mesh.shape["pipe"], 2, 2, 4, 4), AXES)
    tensor, dp, all_model = ("h", "c"), ("z", "y"), ("h", "c", "z", "y")
    placed = (
        P(None, dp, tensor),
        P("p", all_model, None),
        P("p", None, all_model),
        P(None, dp, tensor),
    )
    return jax.shard_map(
        on_device,
        mesh=split,
        in_specs=placed,
        out_specs=(P("p", all_model, None), P("p", None, all_model), P()),
        check_vma=False,
    )
```

```python
import functools

import jax
import jax.numpy as jnp
from jax import lax
from jax.experimental import pallas as pl
from jax.experimental.pallas import tpu as pltpu
from jax.sharding import Mesh
from jax.sharding import PartitionSpec as P


CLIP_NORM = 16384
AXES = ("p", "h", "c", "z", "y")
BF = jnp.bfloat16
F32 = jnp.float32


def dot(a, b):
    return jnp.dot(a, b, preferred_element_type=F32)


def dot_t0(a, b):
    return lax.dot_general(a, b, (((0,), (0,)), ((), ())), preferred_element_type=F32)


def dot_t1(a, b):
    return lax.dot_general(a, b, (((1,), (1,)), ((), ())), preferred_element_type=F32)


def a2a(value, axes):
    return lax.all_to_all(value, axes, 0, 0, tiled=True)


def shift(value, axis, by):
    count = lax.axis_size(axis)
    return lax.ppermute(value, axis, [(i, (i + by) % count) for i in range(count)])


def shift_x(value, by):
    pairs = []
    for p in range(2):
        for h in range(2):
            to = (h * 2 + p + by) % 4
            pairs.append((p * 2 + h, (to % 2) * 2 + to // 2))
    return lax.ppermute(value, ("p", "h"), pairs)


def silu_bf(pre):
    return jax.nn.silu(pre).astype(BF)


def slope_bf(up, pre):
    s = jax.nn.sigmoid(pre)
    return (up * s * (1.0 + pre * (1.0 - s))).astype(BF)


def cut_kernel(along_z, at_ref, one_ref, two_ref, *outs):
    p, x, c, z, y = (at_ref[i] for i in range(5))
    tok = one_ref.shape[0]
    own = one_ref.shape[1] // 16
    half, part = tok // 2, tok // 8
    for rc in range(2):
        for q in range(4):
            source = lax.rem(c + rc, 2) * half + lax.rem(x + 4 - q, 4) * part
            rows = pl.ds(pl.multiple_of(source, part), part)
            to = rc * half + q * part
            for k in range(4):
                for j in range(4):
                    if along_z:
                        zz, yy = lax.rem(z + k, 4), lax.rem(y + 4 - j, 4)
                    else:
                        zz, yy = lax.rem(z + 4 - j, 4), lax.rem(y + k, 4)
                    cols = pl.ds(pl.multiple_of((zz * 4 + yy) * own, own), own)
                    got = jnp.where(p == 0, one_ref[rows, cols], two_ref[rows, cols])
                    outs[k][to : to + part, j * own : (j + 1) * own] = got


def cut(at, one, two, along_z):
    tok, width = one.shape
    vmem = pl.BlockSpec(memory_space=pltpu.VMEM)
    return pl.pallas_call(
        functools.partial(cut_kernel, along_z),
        out_shape=[jax.ShapeDtypeStruct((tok, width // 4), BF)] * 4,
        in_specs=[pl.BlockSpec(memory_space=pltpu.SMEM), vmem, vmem],
        out_specs=[vmem] * 4,
        name="cut_z" if along_z else "cut_y",
    )(at, one, two)


def project_kernel(*refs):
    blocks, weights, sent, kept = refs[:4], refs[4:8], refs[8], refs[9]
    half = blocks[0].shape[0] // 2
    own = weights[0].shape[0]
    for rc, out in ((1, sent), (0, kept)):
        left = jnp.concatenate([b[rc * half : (rc + 1) * half, :] for b in blocks])
        total = dot(left[:, :own], weights[0][...])
        for j in range(1, 4):
            total += dot(left[:, j * own : (j + 1) * own], weights[j][...])
        out[...] = total.astype(out.dtype)


def project(blocks, weights):
    tok, wide = blocks[0].shape
    own, hidden = weights[0].shape
    tile = hidden // 4
    return pl.pallas_call(
        project_kernel,
        out_shape=[
            jax.ShapeDtypeStruct((2 * tok, hidden), BF),
            jax.ShapeDtypeStruct((2 * tok, hidden), F32),
        ],
        grid=(4,),
        in_specs=[pl.BlockSpec((tok, wide), lambda n: (0, 0))] * 4
        + [pl.BlockSpec((own, tile), lambda n: (0, n))] * 4,
        out_specs=[pl.BlockSpec((2 * tok, tile), lambda n: (0, n))] * 2,
        cost_estimate=pl.CostEstimate(
            flops=8 * tok * wide * hidden, bytes_accessed=8 * tok * wide * 2, transcendentals=0
        ),
    )(*blocks, *weights)


def store_piece(outs, j, total):
    for i in range(4):

        @pl.when(j == i)
        def _(i=i):
            outs[i][...] = total.astype(outs[i].dtype)


def grad_v_kernel(*refs):
    blocks, near, far, outs = refs[:4], refs[4:8], refs[8:12], refs[12:]
    total = None
    for k in range(4):
        right = jnp.concatenate([near[k][...], far[k][...]])
        term = dot_t0(blocks[k][...], right)
        total = term if total is None else total + term
    store_piece(outs, pl.program_id(0), total)


def grad_u_kernel(*refs):
    blocks, near, far = refs[:4], refs[4:8], refs[8:12]
    w_ref, outs = refs[12], refs[13:]
    total = None
    for k in range(4):
        right = jnp.concatenate([near[k][0], far[k][0]])
        factor = jnp.concatenate([near[k][1], far[k][1]])
        left = blocks[k][...].astype(F32) + dot_t1(factor, w_ref[...])
        term = dot_t0(left.astype(BF), right)
        total = term if total is None else total + term
    store_piece(outs, pl.program_id(0), total)


def gradient(kernel, blocks, near, far, weights):
    tok, wide = blocks[0].shape
    own = wide // 4
    hidden = near[0].shape[-1]

    def whole(a):
        return pl.BlockSpec(a.shape, lambda j: (0,) * a.ndim)

    def piece(dtype):
        return jax.ShapeDtypeStruct((own, hidden), dtype)

    fold = [pl.BlockSpec((own, hidden), lambda j: (j, 0))] * len(weights)
    return pl.pallas_call(
        kernel,
        out_shape=[piece(F32)] + [piece(BF)] * 3,
        grid=(4,),
        in_specs=[pl.BlockSpec((tok, own), lambda j: (0, j))] * 4
        + [whole(a) for a in (*near, *far)]
        + fold,
        out_specs=[pl.BlockSpec((own, hidden), lambda j: (0, 0))] * 4,
        cost_estimate=pl.CostEstimate(
            flops=8 * tok * wide * hidden, bytes_accessed=8 * tok * wide * 2, transcendentals=0
        ),
    )(*blocks, *near, *far, *weights)


def gather(value, axis):
    return [value] + [shift(value, axis, k) for k in (1, 2, 3)]


def exchange(pieces, axis, sign):
    return [pieces[0]] + [shift(pieces[k], axis, sign * k) for k in (1, 2, 3)]


def sum_back(blocks, axis):
    parts = exchange([blocks[0]] + [b.astype(BF) for b in blocks[1:]], axis, -1)
    return sum((part.astype(F32) for part in parts[1:]), parts[0])


def on_device(inputs, w_in, w_out, cotangent):
    p, h, c, z, y = (lax.axis_index(a) for a in AXES)
    first = p == 0
    n_micro, rows, cols = inputs.shape
    tok = n_micro * rows
    hidden = w_in.shape[2]
    half = tok // 2
    mine = half // 4

    w_i = w_in[0]
    w_o = w_out[0].T
    w_u = jnp.where(first, w_o, w_i)
    w_v = jnp.where(first, w_i, w_o)
    w_3 = lax.ppermute(w_u, "p", [(0, 1), (1, 0)])
    w_vs = gather(w_v, "y")
    at = jnp.stack([p, h * 2 + p, c, z, y])
    x = inputs.reshape(tok, cols)
    ct = cotangent.reshape(tok, cols)
    vs = list(cut(at, x, ct, True))
    us = list(cut(at, ct, x, False))
    vs[0], us[0], w_3 = lax.optimization_barrier((vs[0], us[0], w_3))
    vs = exchange(vs, "z", 1)
    us = exchange(us, "y", 1)
    w_us = gather(w_u, "z")

    m = dot_t0(jnp.where(first, w_u, w_3), jnp.where(first, w_3, w_u))
    m = lax.dynamic_index_in_dim(m.reshape(2, 16, 2, 2, -1, hidden), p, 2, False)
    m = m.transpose(1, 2, 0, 3, 4).reshape(hidden // 2, hidden).astype(BF)
    m = a2a(m, ("z", "y", "h", "c")).reshape(64, -1, hidden)
    m = m.astype(F32).sum(0).astype(BF)
    m = a2a(jnp.broadcast_to(m[None], (4,) + m.shape), ("p", "h")).reshape(-1, hidden)
    w_us[0], m = lax.optimization_barrier((w_us[0], m))
    m_near = lax.all_gather(m, ("z", "y"), axis=0, tiled=True)
    m_far = shift(m_near, "c", 1)

    def reduced(blocks, weights, axis):
        sent, kept = project(blocks, weights)
        kept = kept + shift(sent, "c", 1).astype(F32)
        return sum_back([kept[k * half : (k + 1) * half] for k in range(4)], axis)

    a_v = reduced(vs, w_vs, "z")
    a_u = reduced(us, w_us, "y")
    a_u, a_v, w_3 = lax.optimization_barrier((a_u, a_v, w_3))
    w_3 = jnp.concatenate(gather(w_3, "z"))

    both = jnp.concatenate([a_u, a_v], 1)
    pieces = [both[(4 - k) % 4 * mine :][:mine] for k in range(4)]
    got = [pieces[0]] + [shift_x(pieces[k].astype(BF), k).astype(F32) for k in (1, 2, 3)]
    same = got[0] + got[2]
    other = got[1] + got[3]
    layer0 = jnp.where(first, same, other)
    layer1 = jnp.where(first, other, same)
    up0, pre0 = layer0[:, :hidden], layer0[:, hidden:]
    pre1, up1 = layer1[:, :hidden], layer1[:, hidden:]
    side = hidden // 2
    act0 = silu_bf(pre0)
    low, high = act0[:, :side], act0[:, side:]
    near, far = jnp.where(c == 0, low, high), jnp.where(c == 0, high, low)
    pre1 = pre1 + dot(near, m_near) + dot(far, m_far)
    act1 = silu_bf(pre1)
    slope1 = slope_bf(up1, pre1)
    near, far = dot_t1(slope1, m_near), dot_t1(slope1, m_far)
    low, high = jnp.where(c == 0, near, far), jnp.where(c == 0, far, near)
    slope0 = slope_bf(up0 + jnp.concatenate([low, high], 1), pre0)

    to_first = jnp.stack([slope0, act0, slope1])
    to_last = jnp.stack([act1, slope1, act0])
    same = jnp.where(first, to_first, to_last)
    other = jnp.where(first, to_last, to_first)
    got = [same, shift_x(other, 1), shift_x(same, 2), shift_x(other, 3)]
    rpq = jnp.concatenate(got, 1)
    r_near = gather(rpq[0], "z")
    pq_near = gather(rpq[1:], "y")
    r_far = [shift(a, "c", 1) for a in r_near]
    pq_far = [shift(a, "c", 1) for a in pq_near]

    g_v = sum_back(gradient(grad_v_kernel, vs, r_near, r_far, ()), "y")
    g_u = sum_back(gradient(grad_u_kernel, us, pq_near, pq_far, (w_3,)), "z")

    squares = jnp.sum(g_u * g_u) + jnp.sum(g_v * g_v)
    for axes, count in ((("z", "y"), 16), (("p", "h", "c"), 8)):
        row = jnp.broadcast_to(squares, (count, 8, 128))
        squares = a2a(row, axes)[:, 0, 0].sum()
    grad_norm = jnp.sqrt(squares)
    factor = jnp.minimum(1.0, CLIP_NORM / grad_norm)
    g_in = jnp.where(first, g_v, g_u) * factor
    g_out = jnp.where(first, g_u, g_v) * factor
    return (g_in[None], g_out.T[None], grad_norm)


def solution(mesh):
    split = Mesh(mesh.devices.reshape(mesh.shape["pipe"], 2, 2, 4, 4), AXES)
    tensor, dp, all_model = ("h", "c"), ("z", "y"), ("h", "c", "z", "y")
    placed = (
        P(None, dp, tensor),
        P("p", all_model, None),
        P("p", None, all_model),
        P(None, dp, tensor),
    )
    return jax.shard_map(
        on_device,
        mesh=split,
        in_specs=placed,
        out_specs=(P("p", all_model, None), P("p", None, all_model), P()),
        check_vma=False,
    )
```

```python
import jax
import jax.numpy as jnp
from jax import lax
from jax.experimental import pallas as pl
from jax.experimental.pallas import tpu as pltpu
from jax.sharding import Mesh
from jax.sharding import PartitionSpec as P


CLIP_NORM = 16384
AXES = ("p", "h", "c", "z", "y")
BF = jnp.bfloat16
F32 = jnp.float32


def dot(a, b):
    return jnp.dot(a, b, preferred_element_type=F32)


def dot_t0(a, b):
    return lax.dot_general(a, b, (((0,), (0,)), ((), ())), preferred_element_type=F32)


def dot_t1(a, b):
    return lax.dot_general(a, b, (((1,), (1,)), ((), ())), preferred_element_type=F32)


def a2a(value, axes):
    return lax.all_to_all(value, axes, 0, 0, tiled=True)


def shift(value, axis, by):
    count = lax.axis_size(axis)
    return lax.ppermute(value, axis, [(i, (i + by) % count) for i in range(count)])


def shift_x(value, by):
    pairs = []
    for p in range(2):
        for h in range(2):
            to = (h * 2 + p + by) % 4
            pairs.append((p * 2 + h, (to % 2) * 2 + to // 2))
    return lax.ppermute(value, ("p", "h"), pairs)


def silu_bf(pre):
    return jax.nn.silu(pre).astype(BF)


def slope_bf(up, pre):
    s = jax.nn.sigmoid(pre)
    return (up * s * (1.0 + pre * (1.0 - s))).astype(BF)


def cut_kernel(at_ref, x_ref, ct_ref, *outs):
    p, x, c, z, y = (at_ref[i] for i in range(5))
    tok = x_ref.shape[0]
    own = x_ref.shape[1] // 16
    half, part = tok // 2, tok // 8

    def copy(v_ref, u_ref):
        def group(i, carry):
            rc, q = i // 4, lax.rem(i, 4)
            source = lax.rem(c + rc, 2) * half + lax.rem(x + 4 - q, 4) * part
            rows = pl.ds(pl.multiple_of(source, part), part)
            to = pl.ds(pl.multiple_of(i * part, part), part)
            for k in range(4):
                for j in range(4):
                    at_v = lax.rem(z + k, 4) * 4 + lax.rem(y + 4 - j, 4)
                    at_u = lax.rem(z + 4 - j, 4) * 4 + lax.rem(y + k, 4)
                    for out, ref, at in ((outs[k], v_ref, at_v), (outs[4 + k], u_ref, at_u)):
                        cols = pl.ds(pl.multiple_of(at * own, own), own)
                        out[to, j * own : (j + 1) * own] = ref[rows, cols]
            return carry

        lax.fori_loop(0, 8, group, 0)

    @pl.when(p == 0)
    def _():
        copy(x_ref, ct_ref)

    @pl.when(p != 0)
    def _():
        copy(ct_ref, x_ref)


def cut(at, x, ct):
    tok, width = x.shape
    vmem = pl.BlockSpec(memory_space=pltpu.VMEM)
    outs = pl.pallas_call(
        cut_kernel,
        out_shape=[jax.ShapeDtypeStruct((tok, width // 4), BF)] * 8,
        in_specs=[pl.BlockSpec(memory_space=pltpu.SMEM), vmem, vmem],
        out_specs=[vmem] * 8,
        name="cut",
    )(at, x, ct)
    return list(outs[:4]), list(outs[4:])


def project_kernel(*refs):
    blocks, weights, sent, kept, left = refs[:4], refs[4:8], refs[8], refs[9], refs[10]
    tok = blocks[0].shape[0]
    half = tok // 2

    @pl.when(pl.program_id(0) == 0)
    def _():
        for k in range(4):
            left[k * half : (k + 1) * half, :] = blocks[k][half:, :]
            left[2 * tok + k * half : 2 * tok + (k + 1) * half, :] = blocks[k][:half, :]

    right = jnp.concatenate([w[...] for w in weights])
    sent[...] = dot(left[: 2 * tok, :], right).astype(BF)
    kept[...] = dot(left[2 * tok :, :], right)


def project(blocks, weights):
    tok, wide = blocks[0].shape
    own, hidden = weights[0].shape
    tile = hidden // 4
    return pl.pallas_call(
        project_kernel,
        out_shape=[
            jax.ShapeDtypeStruct((2 * tok, hidden), BF),
            jax.ShapeDtypeStruct((2 * tok, hidden), F32),
        ],
        grid=(4,),
        in_specs=[pl.BlockSpec((tok, wide), lambda n: (0, 0))] * 4
        + [pl.BlockSpec((own, tile), lambda n: (0, n))] * 4,
        out_specs=[pl.BlockSpec((2 * tok, tile), lambda n: (0, n))] * 2,
        scratch_shapes=[pltpu.VMEM((4 * tok, wide), BF)],
        cost_estimate=pl.CostEstimate(
            flops=8 * tok * wide * hidden, bytes_accessed=8 * tok * wide * 2, transcendentals=0
        ),
    )(*blocks, *weights)


def store_piece(outs, j, total):
    for i in range(4):

        @pl.when(j == i)
        def _(i=i):
            outs[i][...] = total.astype(outs[i].dtype)


def fill(scratch, near, far, part=None):
    half = near[0].shape[-2]
    for k in range(4):
        for i, ref in enumerate((near[k], far[k])):
            to = (2 * k + i) * half
            scratch[to : to + half, :] = ref[...] if part is None else ref[part]


def grad_v_kernel(*refs):
    blocks, near, far, outs, right = refs[:4], refs[4:8], refs[8:12], refs[12:16], refs[16]

    @pl.when(pl.program_id(0) == 0)
    def _():
        fill(right, near, far)

    left = jnp.concatenate([b[...] for b in blocks])
    store_piece(outs, pl.program_id(0), dot_t0(left, right[...]))


def grad_u_kernel(*refs):
    blocks, near, far, w_refs = refs[:4], refs[4:8], refs[8:12], refs[12:16]
    outs, right, factor, fold = refs[16:20], refs[20], refs[21], refs[22]
    j = pl.program_id(0)

    @pl.when(j == 0)
    def _():
        fill(right, near, far, 0)
        fill(factor, near, far, 1)

    for i in range(4):

        @pl.when(j == i)
        def _(i=i):
            fold[...] = w_refs[i][...]

    left = jnp.concatenate([b[...] for b in blocks]).astype(F32)
    left = (left + dot_t1(factor[...], fold[...])).astype(BF)
    store_piece(outs, j, dot_t0(left, right[...]))


def gradient(kernel, blocks, near, far, weights):
    tok, wide = blocks[0].shape
    own = wide // 4
    hidden = near[0].shape[-1]

    def whole(a):
        return pl.BlockSpec(a.shape, lambda j: (0,) * a.ndim)

    def piece(dtype):
        return jax.ShapeDtypeStruct((own, hidden), dtype)

    scratch = [pltpu.VMEM((4 * tok, hidden), BF)]
    if weights:
        scratch += [pltpu.VMEM((4 * tok, hidden), BF), pltpu.VMEM((own, hidden), BF)]
    return pl.pallas_call(
        kernel,
        out_shape=[piece(F32)] + [piece(BF)] * 3,
        grid=(4,),
        in_specs=[pl.BlockSpec((tok, own), lambda j: (0, j))] * 4
        + [whole(a) for a in (*near, *far, *weights)],
        out_specs=[pl.BlockSpec((own, hidden), lambda j: (0, 0))] * 4,
        scratch_shapes=scratch,
        cost_estimate=pl.CostEstimate(
            flops=8 * tok * wide * hidden, bytes_accessed=8 * tok * wide * 2, transcendentals=0
        ),
    )(*blocks, *near, *far, *weights)


def gather(value, axis):
    return [value] + [shift(value, axis, k) for k in (1, 2, 3)]


def exchange(pieces, axis, sign):
    return [pieces[0]] + [shift(pieces[k], axis, sign * k) for k in (1, 2, 3)]


def sum_back(blocks, axis):
    parts = exchange([blocks[0]] + [b.astype(BF) for b in blocks[1:]], axis, -1)
    return sum((part.astype(F32) for part in parts[1:]), parts[0])


def on_device(inputs, w_in, w_out, cotangent):
    p, h, c, z, y = (lax.axis_index(a) for a in AXES)
    first = p == 0
    n_micro, rows, cols = inputs.shape
    tok = n_micro * rows
    hidden = w_in.shape[2]
    half = tok // 2
    mine = half // 4

    w_i = w_in[0]
    w_o = w_out[0].T
    w_u = jnp.where(first, w_o, w_i)
    w_v = jnp.where(first, w_i, w_o)
    w_3 = lax.ppermute(w_u, "p", [(0, 1), (1, 0)])
    w_vs = gather(w_v, "y")
    at = jnp.stack([p, h * 2 + p, c, z, y])
    vs, us = cut(at, inputs.reshape(tok, cols), cotangent.reshape(tok, cols))
    vs = exchange(vs, "z", 1)
    us = exchange(us, "y", 1)
    w_us = gather(w_u, "z")

    m = 0.0
    far_u, far_3 = shift(w_u, "c", 1), shift(w_3, "c", 1)
    for mine_u, mine_3 in ((w_u, w_3), (far_u, far_3)):
        m += dot_t0(jnp.where(first, mine_u, mine_3), jnp.where(first, mine_3, mine_u))
    m = lax.dynamic_slice(
        m.reshape(2, 16, 2, -1, hidden), (c, 0, p, 0, 0), (1, 16, 1, hidden // 64, hidden)
    )
    m = a2a(m.reshape(hidden // 4, hidden).astype(BF), ("z", "y", "h"))
    m = m.reshape(32, -1, hidden).astype(F32).sum(0).astype(BF)
    m = a2a(jnp.broadcast_to(m[None], (4,) + m.shape), ("p", "h")).reshape(-1, hidden)
    w_us[0], m = lax.optimization_barrier((w_us[0], m))
    m_near = lax.all_gather(m, ("z", "y"), axis=0, tiled=True)
    m_far = shift(m_near, "c", 1)

    def reduced(blocks, weights, axis):
        sent, kept = project(blocks, weights)
        kept = kept + shift(sent, "c", 1).astype(F32)
        return sum_back([kept[k * half : (k + 1) * half] for k in range(4)], axis)

    a_v = reduced(vs, w_vs, "z")
    a_u = reduced(us, w_us, "y")
    w_3s = gather(w_3, "z")

    both = jnp.concatenate([a_u, a_v], 1)
    pieces = [both[(4 - k) % 4 * mine :][:mine] for k in range(4)]
    got = [pieces[0]] + [shift_x(pieces[k].astype(BF), k).astype(F32) for k in (1, 2, 3)]
    same = got[0] + got[2]
    other = got[1] + got[3]
    layer0 = jnp.where(first, same, other)
    layer1 = jnp.where(first, other, same)
    up0, pre0 = layer0[:, :hidden], layer0[:, hidden:]
    pre1, up1 = layer1[:, :hidden], layer1[:, hidden:]
    side = hidden // 2
    act0 = silu_bf(pre0)
    low, high = act0[:, :side], act0[:, side:]
    near, far = jnp.where(c == 0, low, high), jnp.where(c == 0, high, low)
    pre1 = pre1 + dot(near, m_near) + dot(far, m_far)
    act1 = silu_bf(pre1)
    slope1 = slope_bf(up1, pre1)
    near, far = dot_t1(slope1, m_near), dot_t1(slope1, m_far)
    low, high = jnp.where(c == 0, near, far), jnp.where(c == 0, far, near)
    slope0 = slope_bf(up0 + jnp.concatenate([low, high], 1), pre0)

    to_first = jnp.stack([slope0, act0, slope1])
    to_last = jnp.stack([act1, slope1, act0])
    same = jnp.where(first, to_first, to_last)
    other = jnp.where(first, to_last, to_first)
    got = [same, shift_x(other, 1), shift_x(same, 2), shift_x(other, 3)]
    rpq = jnp.concatenate(got, 1)
    r_near = gather(rpq[0], "z")
    pq_near = gather(rpq[1:], "y")
    r_far = [shift(a, "c", 1) for a in r_near]
    pq_far = [shift(a, "c", 1) for a in pq_near]

    g_v = sum_back(gradient(grad_v_kernel, vs, r_near, r_far, ()), "y")
    g_u = sum_back(gradient(grad_u_kernel, us, pq_near, pq_far, w_3s), "z")

    squares = jnp.sum(g_u * g_u) + jnp.sum(g_v * g_v)
    for axes, count in ((("z", "y"), 16), (("p", "h", "c"), 8)):
        row = jnp.broadcast_to(squares, (count, 8, 128))
        squares = a2a(row, axes)[:, 0, 0].sum()
    grad_norm = jnp.sqrt(squares)
    factor = jnp.minimum(1.0, CLIP_NORM / grad_norm)
    g_in = jnp.where(first, g_v, g_u) * factor
    g_out = jnp.where(first, g_u, g_v) * factor
    return (g_in[None], g_out.T[None], grad_norm)


def solution(mesh):
    split = Mesh(mesh.devices.reshape(mesh.shape["pipe"], 2, 2, 4, 4), AXES)
    tensor, dp, all_model = ("h", "c"), ("z", "y"), ("h", "c", "z", "y")
    placed = (
        P(None, dp, tensor),
        P("p", all_model, None),
        P("p", None, all_model),
        P(None, dp, tensor),
    )
    return jax.shard_map(
        on_device,
        mesh=split,
        in_specs=placed,
        out_specs=(P("p", all_model, None), P("p", None, all_model), P()),
        check_vma=False,
    )
```

```python
import jax
import jax.numpy as jnp
from jax import lax
from jax.experimental import pallas as pl
from jax.experimental.pallas import tpu as pltpu
from jax.sharding import Mesh
from jax.sharding import PartitionSpec as P


CLIP_NORM = 16384
AXES = ("p", "h", "c", "z", "y")
BF = jnp.bfloat16
F32 = jnp.float32


def dot(a, b):
    return jnp.dot(a, b, preferred_element_type=F32)


def dot_t0(a, b):
    return lax.dot_general(a, b, (((0,), (0,)), ((), ())), preferred_element_type=F32)


def dot_t1(a, b):
    return lax.dot_general(a, b, (((1,), (1,)), ((), ())), preferred_element_type=F32)


def a2a(value, axes):
    return lax.all_to_all(value, axes, 0, 0, tiled=True)


def shift(value, axis, by):
    count = lax.axis_size(axis)
    return lax.ppermute(value, axis, [(i, (i + by) % count) for i in range(count)])


def shift_x(value, by):
    pairs = []
    for p in range(2):
        for h in range(2):
            to = (h * 2 + p + by) % 4
            pairs.append((p * 2 + h, (to % 2) * 2 + to // 2))
    return lax.ppermute(value, ("p", "h"), pairs)


def silu_bf(pre):
    return jax.nn.silu(pre).astype(BF)


def slope_bf(up, pre):
    s = jax.nn.sigmoid(pre)
    return (up * s * (1.0 + pre * (1.0 - s))).astype(BF)


def cut_kernel(at_ref, x_ref, ct_ref, *outs):
    p, x, c, z, y = (at_ref[i] for i in range(5))
    tok = x_ref.shape[0]
    own = x_ref.shape[1] // 16
    half, part = tok // 2, tok // 8

    def copy(v_ref, u_ref):
        def group(i, carry):
            rc, q = i // 4, lax.rem(i, 4)
            source = lax.rem(c + rc, 2) * half + lax.rem(x + 4 - q, 4) * part
            rows = pl.ds(pl.multiple_of(source, part), part)
            to = pl.ds(pl.multiple_of(i * part, part), part)
            for k in range(4):
                for j in range(4):
                    at_v = lax.rem(z + k, 4) * 4 + lax.rem(y + 4 - j, 4)
                    at_u = lax.rem(z + 4 - j, 4) * 4 + lax.rem(y + k, 4)
                    for out, ref, at in ((outs[k], v_ref, at_v), (outs[4 + k], u_ref, at_u)):
                        cols = pl.ds(pl.multiple_of(at * own, own), own)
                        out[to, j * own : (j + 1) * own] = ref[rows, cols]
            return carry

        lax.fori_loop(0, 8, group, 0)

    @pl.when(p == 0)
    def _():
        copy(x_ref, ct_ref)

    @pl.when(p != 0)
    def _():
        copy(ct_ref, x_ref)


def cut(at, x, ct):
    tok, width = x.shape
    vmem = pl.BlockSpec(memory_space=pltpu.VMEM)
    outs = pl.pallas_call(
        cut_kernel,
        out_shape=[jax.ShapeDtypeStruct((tok, width // 4), BF)] * 8,
        in_specs=[pl.BlockSpec(memory_space=pltpu.SMEM), vmem, vmem],
        out_specs=[vmem] * 8,
        name="cut",
    )(at, x, ct)
    return list(outs[:4]), list(outs[4:])


def project_kernel(*refs):
    blocks, weights, sent, kept, left = refs[:4], refs[4:8], refs[8], refs[9], refs[10]
    tok = blocks[0].shape[0]
    half = tok // 2

    @pl.when(pl.program_id(0) == 0)
    def _():
        for k in range(4):
            left[k * half : (k + 1) * half, :] = blocks[k][half:, :]
            left[2 * tok + k * half : 2 * tok + (k + 1) * half, :] = blocks[k][:half, :]

    right = jnp.concatenate([w[...] for w in weights])
    total = dot(left[...], right)
    sent[...] = total[: 2 * tok].astype(BF)
    kept[...] = total[2 * tok :]


def project(blocks, weights):
    tok, wide = blocks[0].shape
    own, hidden = weights[0].shape
    tile = hidden // 4
    return pl.pallas_call(
        project_kernel,
        out_shape=[
            jax.ShapeDtypeStruct((2 * tok, hidden), BF),
            jax.ShapeDtypeStruct((2 * tok, hidden), F32),
        ],
        grid=(4,),
        in_specs=[pl.BlockSpec((tok, wide), lambda n: (0, 0))] * 4
        + [pl.BlockSpec((own, tile), lambda n: (0, n))] * 4,
        out_specs=[pl.BlockSpec((2 * tok, tile), lambda n: (0, n))] * 2,
        scratch_shapes=[pltpu.VMEM((4 * tok, wide), BF)],
        cost_estimate=pl.CostEstimate(
            flops=8 * tok * wide * hidden, bytes_accessed=8 * tok * wide * 2, transcendentals=0
        ),
    )(*blocks, *weights)


def turn_kernel(*refs):
    blocks, out = refs[:4], refs[4]
    tok = blocks[0].shape[0]
    for k in range(4):
        out[:, k * tok : (k + 1) * tok] = blocks[k][...].T


def turn(blocks):
    tok, wide = blocks[0].shape
    return pl.pallas_call(
        turn_kernel,
        out_shape=jax.ShapeDtypeStruct((wide, 4 * tok), BF),
        grid=(4,),
        in_specs=[pl.BlockSpec((tok, wide // 4), lambda j: (0, j))] * 4,
        out_specs=pl.BlockSpec((wide // 4, 4 * tok), lambda j: (j, 0)),
        cost_estimate=pl.CostEstimate(
            flops=2 * tok * wide * wide, bytes_accessed=16 * tok * wide, transcendentals=0
        ),
    )(*blocks)


def interleave(near, far):
    return jnp.concatenate([piece for pair in zip(near, far) for piece in pair])


def split_rows(outs, total):
    own = outs[0].shape[0]
    for j in range(4):
        outs[j][...] = total[j * own : (j + 1) * own].astype(outs[j].dtype)


def grad_v_kernel(*refs):
    turned, near, far, outs = refs[0], refs[1:5], refs[5:9], refs[9:]
    right = interleave([a[...] for a in near], [a[...] for a in far])
    split_rows(outs, dot(turned[...], right))


def grad_v_call(turned, near, far):
    wide, tok = turned.shape
    half, hidden = near[0].shape
    own, tile = wide // 4, hidden // 4
    return pl.pallas_call(
        grad_v_kernel,
        out_shape=[jax.ShapeDtypeStruct((own, hidden), t) for t in (F32, BF, BF, BF)],
        grid=(4,),
        in_specs=[pl.BlockSpec((wide, tok), lambda n: (0, 0))]
        + [pl.BlockSpec((half, tile), lambda n: (0, n))] * 8,
        out_specs=[pl.BlockSpec((own, tile), lambda n: (0, n))] * 4,
        cost_estimate=pl.CostEstimate(
            flops=2 * tok * wide * hidden, bytes_accessed=8 * tok * wide, transcendentals=0
        ),
        name="grad_v",
    )(turned, *near, *far)


def grad_u_kernel(*refs):
    turned, w_refs, q_refs, p_refs = refs[0], refs[1:5], refs[5:13], refs[13:21]
    outs, fold, factor, left = refs[21:25], refs[25], refs[26], refs[27]
    s = pl.program_id(0)
    own = w_refs[0].shape[0]
    half = q_refs[0].shape[1]
    tile = turned.shape[1]

    @pl.when(s == 0)
    def _():
        for j in range(4):
            fold[j * own : (j + 1) * own, :] = w_refs[j][...]
            for i in range(2):
                to = (2 * j + i) * half
                factor[to : to + half, :] = q_refs[4 * i + j][0]

    @pl.when(s < 4)
    def _():
        at = pl.ds(pl.multiple_of(s * tile, tile), tile)
        total = turned[...].astype(F32) + dot_t1(fold[...], factor[at, :])
        left[:, at] = total.astype(BF)

    @pl.when(s >= 4)
    def _():
        right = interleave([a[0] for a in p_refs[:4]], [a[0] for a in p_refs[4:]])
        split_rows(outs, dot(left[...], right))


def grad_u_call(turned, near, far, weights):
    wide, tok = turned.shape
    half, hidden = near[0].shape[1:]
    own, tile = wide // 4, hidden // 4

    def late(s):
        return jnp.maximum(s - 4, 0)

    return pl.pallas_call(
        grad_u_kernel,
        out_shape=[jax.ShapeDtypeStruct((own, hidden), t) for t in (F32, BF, BF, BF)],
        grid=(8,),
        in_specs=[pl.BlockSpec((wide, tok // 4), lambda s: (0, jnp.minimum(s, 3)))]
        + [pl.BlockSpec((own, hidden), lambda s: (0, 0))] * 4
        + [pl.BlockSpec((1, half, hidden), lambda s: (1, 0, 0))] * 8
        + [pl.BlockSpec((1, half, tile), lambda s: (0, 0, late(s)))] * 8,
        out_specs=[pl.BlockSpec((own, tile), lambda s: (0, late(s)))] * 4,
        scratch_shapes=[
            pltpu.VMEM((wide, hidden), BF),
            pltpu.VMEM((tok, hidden), BF),
            pltpu.VMEM((wide, tok), BF),
        ],
        cost_estimate=pl.CostEstimate(
            flops=4 * tok * wide * hidden, bytes_accessed=16 * tok * wide, transcendentals=0
        ),
        name="grad_u",
    )(turned, *weights, *near, *far, *near, *far)


def gather(value, axis):
    return [value] + [shift(value, axis, k) for k in (1, 2, 3)]


def exchange(pieces, axis, sign):
    return [pieces[0]] + [shift(pieces[k], axis, sign * k) for k in (1, 2, 3)]


def sum_back(blocks, axis):
    parts = exchange([blocks[0]] + [b.astype(BF) for b in blocks[1:]], axis, -1)
    return sum((part.astype(F32) for part in parts[1:]), parts[0])


def on_device(inputs, w_in, w_out, cotangent):
    p, h, c, z, y = (lax.axis_index(a) for a in AXES)
    first = p == 0
    n_micro, rows, cols = inputs.shape
    tok = n_micro * rows
    hidden = w_in.shape[2]
    half = tok // 2
    mine = half // 4

    w_i = w_in[0]
    w_o = w_out[0].T
    w_u = jnp.where(first, w_o, w_i)
    w_v = jnp.where(first, w_i, w_o)
    w_3 = lax.ppermute(w_u, "p", [(0, 1), (1, 0)])
    w_vs = gather(w_v, "y")
    at = jnp.stack([p, h * 2 + p, c, z, y])
    vs, us = cut(at, inputs.reshape(tok, cols), cotangent.reshape(tok, cols))
    vs = exchange(vs, "z", 1)
    us = exchange(us, "y", 1)
    w_us = gather(w_u, "z")

    m = 0.0
    far_u, far_3 = shift(w_u, "c", 1), shift(w_3, "c", 1)
    for mine_u, mine_3 in ((w_u, w_3), (far_u, far_3)):
        m += dot_t0(jnp.where(first, mine_u, mine_3), jnp.where(first, mine_3, mine_u))
    m = lax.dynamic_slice(
        m.reshape(2, 16, 2, -1, hidden), (c, 0, p, 0, 0), (1, 16, 1, hidden // 64, hidden)
    )
    m = a2a(m.reshape(hidden // 4, hidden).astype(BF), ("z", "y", "h"))
    m = m.reshape(32, -1, hidden).astype(F32).sum(0).astype(BF)
    m = a2a(jnp.broadcast_to(m[None], (4,) + m.shape), ("p", "h")).reshape(-1, hidden)
    w_us[0], w_vs[0], m = lax.optimization_barrier((w_us[0], w_vs[0], m))
    m_near = lax.all_gather(m, ("z", "y"), axis=0, tiled=True)
    m_far = shift(m_near, "c", 1)

    def reduced(blocks, weights, axis):
        sent, kept = project(blocks, weights)
        sent = shift(sent, "c", 1)
        kept = kept + sent.astype(F32)
        return sum_back([kept[k * half : (k + 1) * half] for k in range(4)], axis)

    a_v = reduced(vs, w_vs, "z")
    a_u = reduced(us, w_us, "y")
    w_3s = gather(w_3, "z")

    both = jnp.concatenate([a_u, a_v], 1)
    pieces = [both[(4 - k) % 4 * mine :][:mine] for k in range(4)]
    got = [pieces[0]] + [shift_x(pieces[k].astype(BF), k).astype(F32) for k in (1, 2, 3)]
    same = got[0] + got[2]
    other = got[1] + got[3]
    layer0 = jnp.where(first, same, other)
    layer1 = jnp.where(first, other, same)
    up0, pre0 = layer0[:, :hidden], layer0[:, hidden:]
    pre1, up1 = layer1[:, :hidden], layer1[:, hidden:]
    side = hidden // 2
    act0 = silu_bf(pre0)
    low, high = act0[:, :side], act0[:, side:]
    near, far = jnp.where(c == 0, low, high), jnp.where(c == 0, high, low)
    pre1 = pre1 + dot(near, m_near) + dot(far, m_far)
    act1 = silu_bf(pre1)
    slope1 = slope_bf(up1, pre1)
    near, far = dot_t1(slope1, m_near), dot_t1(slope1, m_far)
    low, high = jnp.where(c == 0, near, far), jnp.where(c == 0, far, near)
    slope0 = slope_bf(up0 + jnp.concatenate([low, high], 1), pre0)

    to_first = jnp.stack([slope0, act0, slope1])
    to_last = jnp.stack([act1, slope1, act0])
    same = jnp.where(first, to_first, to_last)
    other = jnp.where(first, to_last, to_first)
    got = [same, shift_x(other, 1), shift_x(same, 2), shift_x(other, 3)]
    rpq = jnp.concatenate(got, 1)
    r_near = gather(rpq[0], "z")
    pq_near = gather(rpq[1:], "y")
    r_far = [shift(a, "c", 1) for a in r_near]
    pq_far = [shift(a, "c", 1) for a in pq_near]

    g_v = sum_back(grad_v_call(turn(vs), r_near, r_far), "y")
    g_u = sum_back(grad_u_call(turn(us), pq_near, pq_far, w_3s), "z")

    squares = jnp.sum(g_u * g_u) + jnp.sum(g_v * g_v)
    for axes, count in ((("z", "y"), 16), (("p", "h", "c"), 8)):
        row = jnp.broadcast_to(squares, (count, 8, 128))
        squares = a2a(row, axes)[:, 0, 0].sum()
    grad_norm = jnp.sqrt(squares)
    factor = jnp.minimum(1.0, CLIP_NORM / grad_norm)
    g_in = jnp.where(first, g_v, g_u) * factor
    g_out = jnp.where(first, g_u, g_v) * factor
    return (g_in[None], g_out.T[None], grad_norm)


def solution(mesh):
    split = Mesh(mesh.devices.reshape(mesh.shape["pipe"], 2, 2, 4, 4), AXES)
    tensor, dp, all_model = ("h", "c"), ("z", "y"), ("h", "c", "z", "y")
    placed = (
        P(None, dp, tensor),
        P("p", all_model, None),
        P("p", None, all_model),
        P(None, dp, tensor),
    )
    return jax.shard_map(
        on_device,
        mesh=split,
        in_specs=placed,
        out_specs=(P("p", all_model, None), P("p", None, all_model), P()),
        check_vma=False,
    )
```

```python
import jax
import jax.numpy as jnp
from jax import lax
from jax.experimental import pallas as pl
from jax.experimental.pallas import tpu as pltpu
from jax.sharding import Mesh
from jax.sharding import PartitionSpec as P


CLIP_NORM = 16384
AXES = ("p", "h", "c", "z", "y")
BF = jnp.bfloat16
F32 = jnp.float32


def dot(a, b):
    return jnp.dot(a, b, preferred_element_type=F32)


def dot_t0(a, b):
    return lax.dot_general(a, b, (((0,), (0,)), ((), ())), preferred_element_type=F32)


def dot_t1(a, b):
    return lax.dot_general(a, b, (((1,), (1,)), ((), ())), preferred_element_type=F32)


def a2a(value, axes):
    return lax.all_to_all(value, axes, 0, 0, tiled=True)


def shift(value, axis, by):
    count = lax.axis_size(axis)
    return lax.ppermute(value, axis, [(i, (i + by) % count) for i in range(count)])


def shift_x(value, by):
    pairs = []
    for p in range(2):
        for h in range(2):
            to = (h * 2 + p + by) % 4
            pairs.append((p * 2 + h, (to % 2) * 2 + to // 2))
    return lax.ppermute(value, ("p", "h"), pairs)


def silu_bf(pre):
    return jax.nn.silu(pre).astype(BF)


def slope_bf(up, pre):
    s = jax.nn.sigmoid(pre)
    return (up * s * (1.0 + pre * (1.0 - s))).astype(BF)


def cut_kernel(at_ref, x_ref, ct_ref, *outs):
    p, x, c, z, y = (at_ref[i] for i in range(5))
    tok = x_ref.shape[0]
    own = x_ref.shape[1] // 16
    half, part = tok // 2, tok // 8

    def copy(v_ref, u_ref):
        def group(i, carry):
            rc, q = i // 4, lax.rem(i, 4)
            source = lax.rem(c + rc, 2) * half + lax.rem(x + 4 - q, 4) * part
            rows = pl.ds(pl.multiple_of(source, part), part)
            to = pl.ds(pl.multiple_of(i * part, part), part)
            for k in range(4):
                for j in range(4):
                    at_v = lax.rem(z + k, 4) * 4 + lax.rem(y + 4 - j, 4)
                    at_u = lax.rem(z + 4 - j, 4) * 4 + lax.rem(y + k, 4)
                    for out, ref, at in ((outs[k], v_ref, at_v), (outs[4 + k], u_ref, at_u)):
                        cols = pl.ds(pl.multiple_of(at * own, own), own)
                        out[to, j * own : (j + 1) * own] = ref[rows, cols]
            return carry

        lax.fori_loop(0, 8, group, 0)

    @pl.when(p == 0)
    def _():
        copy(x_ref, ct_ref)

    @pl.when(p != 0)
    def _():
        copy(ct_ref, x_ref)


def cut(at, x, ct):
    tok, width = x.shape
    vmem = pl.BlockSpec(memory_space=pltpu.VMEM)
    outs = pl.pallas_call(
        cut_kernel,
        out_shape=[jax.ShapeDtypeStruct((tok, width // 4), BF)] * 8,
        in_specs=[pl.BlockSpec(memory_space=pltpu.SMEM), vmem, vmem],
        out_specs=[vmem] * 8,
        name="cut",
    )(at, x, ct)
    return list(outs[:4]), list(outs[4:])


def project_kernel(*refs):
    blocks, weights, sent, kept, left = refs[:4], refs[4:8], refs[8], refs[9], refs[10]
    tok = blocks[0].shape[0]
    half = tok // 2

    @pl.when(pl.program_id(0) == 0)
    def _():
        for k in range(4):
            left[k * half : (k + 1) * half, :] = blocks[k][half:, :]
            left[2 * tok + k * half : 2 * tok + (k + 1) * half, :] = blocks[k][:half, :]

    right = jnp.concatenate([w[...] for w in weights])
    total = dot(left[...], right)
    sent[...] = total[: 2 * tok].astype(BF)
    kept[...] = total[2 * tok :]


def project(blocks, weights):
    tok, wide = blocks[0].shape
    own, hidden = weights[0].shape
    tile = hidden // 4
    return pl.pallas_call(
        project_kernel,
        out_shape=[
            jax.ShapeDtypeStruct((2 * tok, hidden), BF),
            jax.ShapeDtypeStruct((2 * tok, hidden), F32),
        ],
        grid=(4,),
        in_specs=[pl.BlockSpec((tok, wide), lambda n: (0, 0))] * 4
        + [pl.BlockSpec((own, tile), lambda n: (0, n))] * 4,
        out_specs=[pl.BlockSpec((2 * tok, tile), lambda n: (0, n))] * 2,
        scratch_shapes=[pltpu.VMEM((4 * tok, wide), BF)],
        cost_estimate=pl.CostEstimate(
            flops=8 * tok * wide * hidden, bytes_accessed=8 * tok * wide * 2, transcendentals=0
        ),
    )(*blocks, *weights)


def turn_kernel(*refs):
    blocks, out = refs[:4], refs[4]
    tok = blocks[0].shape[0]
    half = tok // 2
    for rc in range(2):
        for k in range(4):
            to = (rc * 4 + k) * half
            out[:, to : to + half] = blocks[k][rc * half : (rc + 1) * half, :].T


def turn(blocks):
    tok, wide = blocks[0].shape
    return pl.pallas_call(
        turn_kernel,
        out_shape=jax.ShapeDtypeStruct((wide, 4 * tok), BF),
        grid=(4,),
        in_specs=[pl.BlockSpec((tok, wide // 4), lambda j: (0, j))] * 4,
        out_specs=pl.BlockSpec((wide // 4, 4 * tok), lambda j: (j, 0)),
        cost_estimate=pl.CostEstimate(
            flops=2 * tok * wide * wide, bytes_accessed=16 * tok * wide, transcendentals=0
        ),
    )(*blocks)


def split_rows(outs, total):
    own = outs[0].shape[0]
    for j in range(4):
        outs[j][...] = total[j * own : (j + 1) * own].astype(outs[j].dtype)


def grad_v_kernel(turned, *refs):
    right = jnp.concatenate([piece[...] for piece in refs[:8]])
    split_rows(refs[8:], dot(turned[...], right))


def grad_v_call(turned, pieces):
    wide, tok = turned.shape
    half, hidden = pieces[0].shape
    own, tile = wide // 4, hidden // 4
    return pl.pallas_call(
        grad_v_kernel,
        out_shape=[jax.ShapeDtypeStruct((own, hidden), t) for t in (F32, BF, BF, BF)],
        grid=(4,),
        in_specs=[pl.BlockSpec((wide, tok), lambda n: (0, 0))]
        + [pl.BlockSpec((half, tile), lambda n: (0, n))] * 8,
        out_specs=[pl.BlockSpec((own, tile), lambda n: (0, n))] * 4,
        cost_estimate=pl.CostEstimate(
            flops=2 * tok * wide * hidden, bytes_accessed=8 * tok * wide, transcendentals=0
        ),
        name="grad_v",
    )(turned, *pieces)


def grad_u_kernel(at_ref, turned, *refs):
    w_refs, acts, slopes, outs = refs[:4], refs[4:12], refs[12:20], refs[20:24]
    fold, factor, right, left = refs[24:]
    s = pl.program_id(0)
    own = w_refs[0].shape[0]
    half = acts[0].shape[0]
    tile = turned.shape[1]
    first = at_ref[0] == 0

    @pl.when(s == 0)
    def _():
        for j in range(4):
            fold[j * own : (j + 1) * own, :] = w_refs[j][...]
        for i in range(8):
            act, slope = acts[i][...], slopes[i][...]
            right[i * half : (i + 1) * half, :] = jnp.where(first, act, slope)
            factor[i * half : (i + 1) * half, :] = jnp.where(first, slope, act)

    @pl.when(s < 4)
    def _():
        at = pl.ds(pl.multiple_of(s * tile, tile), tile)
        total = turned[...].astype(F32) + dot_t1(fold[...], factor[at, :])
        left[:, at] = total.astype(BF)

    @pl.when(s >= 4)
    def _():
        width = outs[0].shape[1]
        at = pl.ds(pl.multiple_of((s - 4) * width, width), width)
        split_rows(outs, dot(left[...], right[:, at]))


def grad_u_call(at, turned, act, slope, weights):
    wide, tok = turned.shape
    hidden = act[0].shape[1]
    own, tile = wide // 4, hidden // 4

    def late(s):
        return jnp.maximum(s - 4, 0)

    return pl.pallas_call(
        grad_u_kernel,
        out_shape=[jax.ShapeDtypeStruct((own, hidden), t) for t in (F32, BF, BF, BF)],
        grid=(8,),
        in_specs=[pl.BlockSpec(memory_space=pltpu.SMEM)]
        + [pl.BlockSpec((wide, tok // 4), lambda s: (0, jnp.minimum(s, 3)))]
        + [pl.BlockSpec((own, hidden), lambda s: (0, 0))] * 4
        + [pl.BlockSpec((tok // 8, hidden), lambda s: (0, 0))] * 16,
        out_specs=[pl.BlockSpec((own, tile), lambda s: (0, late(s)))] * 4,
        scratch_shapes=[
            pltpu.VMEM((wide, hidden), BF),
            pltpu.VMEM((tok, hidden), BF),
            pltpu.VMEM((tok, hidden), BF),
            pltpu.VMEM((wide, tok), BF),
        ],
        cost_estimate=pl.CostEstimate(
            flops=4 * tok * wide * hidden, bytes_accessed=16 * tok * wide, transcendentals=0
        ),
        name="grad_u",
    )(at, turned, *weights, *act, *slope)


def gather(value, axis):
    return [value] + [shift(value, axis, k) for k in (1, 2, 3)]


def exchange(pieces, axis, sign):
    return [pieces[0]] + [shift(pieces[k], axis, sign * k) for k in (1, 2, 3)]


def sum_back(blocks, axis):
    parts = exchange([blocks[0]] + [b.astype(BF) for b in blocks[1:]], axis, -1)
    return sum((part.astype(F32) for part in parts[1:]), parts[0])


def on_device(inputs, w_in, w_out, cotangent):
    p, h, c, z, y = (lax.axis_index(a) for a in AXES)
    first = p == 0
    n_micro, rows, cols = inputs.shape
    tok = n_micro * rows
    hidden = w_in.shape[2]
    half = tok // 2
    mine = half // 4

    w_i = w_in[0]
    w_o = w_out[0].T
    w_u = jnp.where(first, w_o, w_i)
    w_v = jnp.where(first, w_i, w_o)
    w_3 = lax.ppermute(w_u, "p", [(0, 1), (1, 0)])
    w_vs = gather(w_v, "y")
    at = jnp.stack([p, h * 2 + p, c, z, y])
    vs, us = cut(at, inputs.reshape(tok, cols), cotangent.reshape(tok, cols))
    vs = exchange(vs, "z", 1)
    us = exchange(us, "y", 1)
    w_us = gather(w_u, "z")

    m = 0.0
    far_u, far_3 = shift(w_u, "c", 1), shift(w_3, "c", 1)
    for mine_u, mine_3 in ((w_u, w_3), (far_u, far_3)):
        m += dot_t0(jnp.where(first, mine_u, mine_3), jnp.where(first, mine_3, mine_u))
    m = lax.dynamic_slice(
        m.reshape(2, 16, 2, -1, hidden), (c, 0, p, 0, 0), (1, 16, 1, hidden // 64, hidden)
    )
    m = a2a(m.reshape(hidden // 4, hidden).astype(BF), ("z", "y", "h"))
    m = m.reshape(32, -1, hidden).astype(F32).sum(0).astype(BF)
    m = a2a(jnp.broadcast_to(m[None], (4,) + m.shape), ("p", "h")).reshape(-1, hidden)
    w_us[0], w_vs[0], m = lax.optimization_barrier((w_us[0], w_vs[0], m))
    m_near = lax.all_gather(m, ("z", "y"), axis=0, tiled=True)
    m_far = shift(m_near, "c", 1)

    def reduced(blocks, weights, axis):
        sent, kept = project(blocks, weights)
        sent = shift(sent, "c", 1)
        kept = kept + sent.astype(F32)
        return sum_back([kept[k * half : (k + 1) * half] for k in range(4)], axis)

    a_v = reduced(vs, w_vs, "z")
    a_u = reduced(us, w_us, "y")
    w_3s = gather(w_3, "z")

    both = jnp.concatenate([a_u, a_v], 1)
    pieces = [both[(4 - k) % 4 * mine :][:mine] for k in range(4)]
    got = [pieces[0]] + [shift_x(pieces[k].astype(BF), k).astype(F32) for k in (1, 2, 3)]
    same = got[0] + got[2]
    other = got[1] + got[3]
    layer0 = jnp.where(first, same, other)
    layer1 = jnp.where(first, other, same)
    up0, pre0 = layer0[:, :hidden], layer0[:, hidden:]
    pre1, up1 = layer1[:, :hidden], layer1[:, hidden:]
    side = hidden // 2
    act0 = silu_bf(pre0)
    act_near = jnp.concatenate([act0] + [shift_x(act0, k) for k in (1, 2, 3)])
    act_near = gather(act_near, "y")
    act_near += [shift(a, "c", 1) for a in act_near]
    low, high = act0[:, :side], act0[:, side:]
    near, far = jnp.where(c == 0, low, high), jnp.where(c == 0, high, low)
    pre1 = pre1 + dot(near, m_near) + dot(far, m_far)
    act1 = silu_bf(pre1)
    slope1 = slope_bf(up1, pre1)
    near, far = dot_t1(slope1, m_near), dot_t1(slope1, m_far)
    low, high = jnp.where(c == 0, near, far), jnp.where(c == 0, far, near)
    slope0 = slope_bf(up0 + jnp.concatenate([low, high], 1), pre0)

    same = jnp.stack([jnp.where(first, slope0, act1), slope1])
    other = jnp.stack([jnp.where(first, act1, slope0), slope1])
    got = [same, shift_x(other, 1), shift_x(same, 2), shift_x(other, 3)]
    r_near = jnp.concatenate([g[0] for g in got])
    s_near = jnp.concatenate([g[1] for g in got])
    r_near = gather(r_near, "z")
    s_near = gather(s_near, "y")
    r_near += [shift(a, "c", 1) for a in r_near]
    s_near += [shift(a, "c", 1) for a in s_near]

    g_v = sum_back(grad_v_call(turn(vs), r_near), "y")
    g_u = sum_back(grad_u_call(at, turn(us), act_near, s_near, w_3s), "z")

    squares = jnp.sum(g_u * g_u) + jnp.sum(g_v * g_v)
    for axes, count in ((("z", "y"), 16), (("p", "h", "c"), 8)):
        row = jnp.broadcast_to(squares, (count, 8, 128))
        squares = a2a(row, axes)[:, 0, 0].sum()
    grad_norm = jnp.sqrt(squares)
    factor = jnp.minimum(1.0, CLIP_NORM / grad_norm)
    g_in = jnp.where(first, g_v, g_u) * factor
    g_out = jnp.where(first, g_u, g_v) * factor
    return (g_in[None], g_out.T[None], grad_norm)


def solution(mesh):
    split = Mesh(mesh.devices.reshape(mesh.shape["pipe"], 2, 2, 4, 4), AXES)
    tensor, dp, all_model = ("h", "c"), ("z", "y"), ("h", "c", "z", "y")
    placed = (
        P(None, dp, tensor),
        P("p", all_model, None),
        P("p", None, all_model),
        P(None, dp, tensor),
    )
    return jax.shard_map(
        on_device,
        mesh=split,
        in_specs=placed,
        out_specs=(P("p", all_model, None), P("p", None, all_model), P()),
        check_vma=False,
    )
```

```python
import jax
import jax.numpy as jnp
from jax import lax
from jax.experimental import pallas as pl
from jax.experimental.pallas import tpu as pltpu
from jax.sharding import Mesh
from jax.sharding import PartitionSpec as P


CLIP_NORM = 16384
AXES = ("p", "h", "c", "z", "y")
BF = jnp.bfloat16
F32 = jnp.float32


def dot(a, b):
    return jnp.dot(a, b, preferred_element_type=F32)


def dot_t0(a, b):
    return lax.dot_general(a, b, (((0,), (0,)), ((), ())), preferred_element_type=F32)


def dot_t1(a, b):
    return lax.dot_general(a, b, (((1,), (1,)), ((), ())), preferred_element_type=F32)


def a2a(value, axes):
    return lax.all_to_all(value, axes, 0, 0, tiled=True)


def shift(value, axis, by):
    count = lax.axis_size(axis)
    return lax.ppermute(value, axis, [(i, (i + by) % count) for i in range(count)])


def shift_x(value, by):
    pairs = []
    for p in range(2):
        for h in range(2):
            to = (h * 2 + p + by) % 4
            pairs.append((p * 2 + h, (to % 2) * 2 + to // 2))
    return lax.ppermute(value, ("p", "h"), pairs)


def silu_bf(pre):
    return jax.nn.silu(pre).astype(BF)


def slope_bf(up, pre):
    s = jax.nn.sigmoid(pre)
    return (up * s * (1.0 + pre * (1.0 - s))).astype(BF)


def cut_kernel(at_ref, x_ref, ct_ref, *outs):
    p, x, c, z, y = (at_ref[i] for i in range(5))
    tok = x_ref.shape[0]
    own = x_ref.shape[1] // 16
    half, part = tok // 2, tok // 8

    def copy(v_ref, u_ref):
        def group(i, carry):
            rc, q = i // 4, lax.rem(i, 4)
            source = lax.rem(c + rc, 2) * half + lax.rem(x + 4 - q, 4) * part
            rows = pl.ds(pl.multiple_of(source, part), part)
            to = pl.ds(pl.multiple_of(i * part, part), part)
            for k in range(4):
                for j in range(4):
                    at_v = lax.rem(z + k, 4) * 4 + lax.rem(y + 4 - j, 4)
                    at_u = lax.rem(z + 4 - j, 4) * 4 + lax.rem(y + k, 4)
                    for out, ref, at in ((outs[k], v_ref, at_v), (outs[4 + k], u_ref, at_u)):
                        cols = pl.ds(pl.multiple_of(at * own, own), own)
                        out[to, j * own : (j + 1) * own] = ref[rows, cols]
            return carry

        lax.fori_loop(0, 8, group, 0)

    @pl.when(p == 0)
    def _():
        copy(x_ref, ct_ref)

    @pl.when(p != 0)
    def _():
        copy(ct_ref, x_ref)


def cut(at, x, ct):
    tok, width = x.shape
    vmem = pl.BlockSpec(memory_space=pltpu.VMEM)
    outs = pl.pallas_call(
        cut_kernel,
        out_shape=[jax.ShapeDtypeStruct((tok, width // 4), BF)] * 8,
        in_specs=[pl.BlockSpec(memory_space=pltpu.SMEM), vmem, vmem],
        out_specs=[vmem] * 8,
        name="cut",
    )(at, x, ct)
    return list(outs[:4]), list(outs[4:])


def project_kernel(*refs):
    blocks, weights, sent, kept, left = refs[:4], refs[4:8], refs[8], refs[9], refs[10]
    tok = blocks[0].shape[0]
    half = tok // 2

    @pl.when(pl.program_id(0) == 0)
    def _():
        for k in range(4):
            left[k * half : (k + 1) * half, :] = blocks[k][half:, :]
            left[2 * tok + k * half : 2 * tok + (k + 1) * half, :] = blocks[k][:half, :]

    right = jnp.concatenate([w[...] for w in weights])
    total = dot(left[...], right)
    sent[...] = total[: 2 * tok].astype(BF)
    kept[...] = total[2 * tok :]


def project(blocks, weights):
    tok, wide = blocks[0].shape
    own, hidden = weights[0].shape
    tile = hidden // 4
    return pl.pallas_call(
        project_kernel,
        out_shape=[
            jax.ShapeDtypeStruct((2 * tok, hidden), BF),
            jax.ShapeDtypeStruct((2 * tok, hidden), F32),
        ],
        grid=(4,),
        in_specs=[pl.BlockSpec((tok, wide), lambda n: (0, 0))] * 4
        + [pl.BlockSpec((own, tile), lambda n: (0, n))] * 4,
        out_specs=[pl.BlockSpec((2 * tok, tile), lambda n: (0, n))] * 2,
        scratch_shapes=[pltpu.VMEM((4 * tok, wide), BF)],
        cost_estimate=pl.CostEstimate(
            flops=8 * tok * wide * hidden, bytes_accessed=8 * tok * wide * 2, transcendentals=0
        ),
    )(*blocks, *weights)


def turn_kernel(*refs):
    blocks, out = refs[:4], refs[4]
    tok = blocks[0].shape[0]
    half = tok // 2
    for rc in range(2):
        for k in range(4):
            to = (rc * 4 + k) * half
            out[:, to : to + half] = blocks[k][rc * half : (rc + 1) * half, :].T


def turn(blocks):
    tok, wide = blocks[0].shape
    return pl.pallas_call(
        turn_kernel,
        out_shape=jax.ShapeDtypeStruct((wide, 4 * tok), BF),
        grid=(4,),
        in_specs=[pl.BlockSpec((tok, wide // 4), lambda j: (0, j))] * 4,
        out_specs=pl.BlockSpec((wide // 4, 4 * tok), lambda j: (j, 0)),
        cost_estimate=pl.CostEstimate(
            flops=2 * tok * wide * wide, bytes_accessed=16 * tok * wide, transcendentals=0
        ),
    )(*blocks)


def split_rows(outs, total):
    own = outs[0].shape[0]
    for j in range(4):
        outs[j][...] = total[j * own : (j + 1) * own].astype(outs[j].dtype)


def grad_v_kernel(turned, *refs):
    right = jnp.concatenate([piece[...] for piece in refs[:8]])
    split_rows(refs[8:], dot(turned[...], right))


def grad_v_call(turned, pieces):
    wide, tok = turned.shape
    half, hidden = pieces[0].shape
    own, tile = wide // 4, hidden // 4
    return pl.pallas_call(
        grad_v_kernel,
        out_shape=[jax.ShapeDtypeStruct((own, hidden), t) for t in (F32, BF, BF, BF)],
        grid=(4,),
        in_specs=[pl.BlockSpec((wide, tok), lambda n: (0, 0))]
        + [pl.BlockSpec((half, tile), lambda n: (0, n))] * 8,
        out_specs=[pl.BlockSpec((own, tile), lambda n: (0, n))] * 4,
        cost_estimate=pl.CostEstimate(
            flops=2 * tok * wide * hidden, bytes_accessed=8 * tok * wide, transcendentals=0
        ),
        name="grad_v",
    )(turned, *pieces)


def grad_u_kernel(at_ref, turned, *refs):
    w_refs, acts, slopes, outs = refs[:4], refs[4:12], refs[12:20], refs[20:24]
    fold, factor, right, left = refs[24:]
    s = pl.program_id(0)
    own = w_refs[0].shape[0]
    half = acts[0].shape[0]
    tile = turned.shape[1]
    first = at_ref[0] == 0

    @pl.when(s == 0)
    def _():
        for j in range(4):
            fold[j * own : (j + 1) * own, :] = w_refs[j][...]
        for i in range(8):
            act, slope = acts[i][...], slopes[i][...]
            right[i * half : (i + 1) * half, :] = jnp.where(first, act, slope)
            factor[i * half : (i + 1) * half, :] = jnp.where(first, slope, act)

    @pl.when(s < 4)
    def _():
        at = pl.ds(pl.multiple_of(s * tile, tile), tile)
        total = turned[...].astype(F32) + dot_t1(fold[...], factor[at, :])
        left[:, at] = total.astype(BF)

    @pl.when(s >= 4)
    def _():
        width = outs[0].shape[1]
        at = pl.ds(pl.multiple_of((s - 4) * width, width), width)
        split_rows(outs, dot(left[...], right[:, at]))


def grad_u_call(at, turned, act, slope, weights):
    wide, tok = turned.shape
    hidden = act[0].shape[1]
    own, tile = wide // 4, hidden // 4

    def late(s):
        return jnp.maximum(s - 4, 0)

    return pl.pallas_call(
        grad_u_kernel,
        out_shape=[jax.ShapeDtypeStruct((own, hidden), t) for t in (F32, BF, BF, BF)],
        grid=(8,),
        in_specs=[pl.BlockSpec(memory_space=pltpu.SMEM)]
        + [pl.BlockSpec((wide, tok // 4), lambda s: (0, jnp.minimum(s, 3)))]
        + [pl.BlockSpec((own, hidden), lambda s: (0, 0))] * 4
        + [pl.BlockSpec((tok // 8, hidden), lambda s: (0, 0))] * 16,
        out_specs=[pl.BlockSpec((own, tile), lambda s: (0, late(s)))] * 4,
        scratch_shapes=[
            pltpu.VMEM((wide, hidden), BF),
            pltpu.VMEM((tok, hidden), BF),
            pltpu.VMEM((tok, hidden), BF),
            pltpu.VMEM((wide, tok), BF),
        ],
        cost_estimate=pl.CostEstimate(
            flops=4 * tok * wide * hidden, bytes_accessed=16 * tok * wide, transcendentals=0
        ),
        name="grad_u",
    )(at, turned, *weights, *act, *slope)


def join_kernel(at_ref, *refs):
    blocks, out = refs[:4], refs[4]
    z, y = at_ref[3], at_ref[4]
    part = blocks[0].shape[0] // 4
    for kz in range(4):
        for ky in range(4):
            to = (lax.rem(z + 4 - kz, 4) * 4 + lax.rem(y + 4 - ky, 4)) * part
            rows = pl.ds(pl.multiple_of(to, part), part)
            out[rows, :] = blocks[kz][ky * part : (ky + 1) * part, :]


def join(at, blocks):
    rows, hidden = blocks[0].shape
    vmem = pl.BlockSpec(memory_space=pltpu.VMEM)
    return pl.pallas_call(
        join_kernel,
        out_shape=jax.ShapeDtypeStruct((4 * rows, hidden), BF),
        in_specs=[pl.BlockSpec(memory_space=pltpu.SMEM)] + [vmem] * 4,
        out_specs=vmem,
        name="join",
    )(at, *blocks)


def gather(value, axis):
    return [value] + [shift(value, axis, k) for k in (1, 2, 3)]


def exchange(pieces, axis, sign):
    return [pieces[0]] + [shift(pieces[k], axis, sign * k) for k in (1, 2, 3)]


def sum_back(blocks, axis):
    parts = exchange([blocks[0]] + [b.astype(BF) for b in blocks[1:]], axis, -1)
    return sum((part.astype(F32) for part in parts[1:]), parts[0])


def on_device(inputs, w_in, w_out, cotangent):
    p, h, c, z, y = (lax.axis_index(a) for a in AXES)
    first = p == 0
    n_micro, rows, cols = inputs.shape
    tok = n_micro * rows
    hidden = w_in.shape[2]
    half = tok // 2
    mine = half // 4

    w_i = w_in[0]
    w_o = w_out[0].T
    w_u = jnp.where(first, w_o, w_i)
    w_v = jnp.where(first, w_i, w_o)
    w_3 = lax.ppermute(w_u, "p", [(0, 1), (1, 0)])
    w_vs = gather(w_v, "y")
    at = jnp.stack([p, h * 2 + p, c, z, y])
    vs, us = cut(at, inputs.reshape(tok, cols), cotangent.reshape(tok, cols))
    vs = exchange(vs, "z", 1)
    us = exchange(us, "y", 1)
    w_us = gather(w_u, "z")

    m = 0.0
    far_u, far_3 = shift(w_u, "c", 1), shift(w_3, "c", 1)
    for mine_u, mine_3 in ((w_u, w_3), (far_u, far_3)):
        m += dot_t0(jnp.where(first, mine_u, mine_3), jnp.where(first, mine_3, mine_u))
    m = lax.dynamic_slice(
        m.reshape(2, 16, 2, -1, hidden), (c, 0, p, 0, 0), (1, 16, 1, hidden // 64, hidden)
    )
    m = a2a(m.reshape(hidden // 4, hidden).astype(BF), ("z", "y", "h"))
    m = m.reshape(32, -1, hidden).astype(F32).sum(0).astype(BF)
    m = a2a(jnp.broadcast_to(m[None], (4,) + m.shape), ("p", "h")).reshape(-1, hidden)
    w_us[0], w_vs[0], m = lax.optimization_barrier((w_us[0], w_vs[0], m))
    m = jnp.concatenate(gather(m, "y"))
    m = gather(m, "z")
    m_near = join(at, m)
    m_far = shift(m_near, "c", 1)

    def reduced(blocks, weights, axis):
        sent, kept = project(blocks, weights)
        sent = shift(sent, "c", 1)
        kept = kept + sent.astype(F32)
        return sum_back([kept[k * half : (k + 1) * half] for k in range(4)], axis)

    a_v = reduced(vs, w_vs, "z")
    a_u = reduced(us, w_us, "y")
    w_3s = gather(w_3, "z")

    both = jnp.concatenate([a_u, a_v], 1)
    pieces = [both[(4 - k) % 4 * mine :][:mine] for k in range(4)]
    got = [pieces[0]] + [shift_x(pieces[k].astype(BF), k).astype(F32) for k in (1, 2, 3)]
    same = got[0] + got[2]
    other = got[1] + got[3]
    layer0 = jnp.where(first, same, other)
    layer1 = jnp.where(first, other, same)
    up0, pre0 = layer0[:, :hidden], layer0[:, hidden:]
    pre1, up1 = layer1[:, :hidden], layer1[:, hidden:]
    side = hidden // 2
    act0 = silu_bf(pre0)
    act_near = jnp.concatenate([act0] + [shift_x(act0, k) for k in (1, 2, 3)])
    act_near = gather(act_near, "y")
    act_near += [shift(a, "c", 1) for a in act_near]
    low, high = act0[:, :side], act0[:, side:]
    near, far = jnp.where(c == 0, low, high), jnp.where(c == 0, high, low)
    pre1 = pre1 + dot(near, m_near) + dot(far, m_far)
    act1 = silu_bf(pre1)
    slope1 = slope_bf(up1, pre1)
    near, far = dot_t1(slope1, m_near), dot_t1(slope1, m_far)
    low, high = jnp.where(c == 0, near, far), jnp.where(c == 0, far, near)
    slope0 = slope_bf(up0 + jnp.concatenate([low, high], 1), pre0)

    same = jnp.stack([jnp.where(first, slope0, act1), slope1])
    other = jnp.stack([jnp.where(first, act1, slope0), slope1])
    got = [same, shift_x(other, 1), shift_x(same, 2), shift_x(other, 3)]
    r_near = jnp.concatenate([g[0] for g in got])
    s_near = jnp.concatenate([g[1] for g in got])
    r_near = gather(r_near, "z")
    s_near = gather(s_near, "y")
    r_near += [shift(a, "c", 1) for a in r_near]
    s_near += [shift(a, "c", 1) for a in s_near]

    g_v = sum_back(grad_v_call(turn(vs), r_near), "y")
    g_u = sum_back(grad_u_call(at, turn(us), act_near, s_near, w_3s), "z")

    squares = jnp.sum(g_u * g_u) + jnp.sum(g_v * g_v)
    for axes, count in ((("z", "y"), 16), (("p", "h", "c"), 8)):
        row = jnp.broadcast_to(squares, (count, 8, 128))
        squares = a2a(row, axes)[:, 0, 0].sum()
    grad_norm = jnp.sqrt(squares)
    factor = jnp.minimum(1.0, CLIP_NORM / grad_norm)
    g_in = jnp.where(first, g_v, g_u) * factor
    g_out = jnp.where(first, g_u, g_v) * factor
    return (g_in[None], g_out.T[None], grad_norm)


def solution(mesh):
    split = Mesh(mesh.devices.reshape(mesh.shape["pipe"], 2, 2, 4, 4), AXES)
    tensor, dp, all_model = ("h", "c"), ("z", "y"), ("h", "c", "z", "y")
    placed = (
        P(None, dp, tensor),
        P("p", all_model, None),
        P("p", None, all_model),
        P(None, dp, tensor),
    )
    return jax.shard_map(
        on_device,
        mesh=split,
        in_specs=placed,
        out_specs=(P("p", all_model, None), P("p", None, all_model), P()),
        check_vma=False,
    )
```

```python
import jax
import jax.numpy as jnp
from jax import lax
from jax.experimental import pallas as pl
from jax.experimental.pallas import tpu as pltpu
from jax.sharding import Mesh
from jax.sharding import PartitionSpec as P


CLIP_NORM = 16384
AXES = ("p", "h", "c", "z", "y")
BF = jnp.bfloat16
F32 = jnp.float32


def dot(a, b):
    return jnp.dot(a, b, preferred_element_type=F32)


def dot_t0(a, b):
    return lax.dot_general(a, b, (((0,), (0,)), ((), ())), preferred_element_type=F32)


def dot_t1(a, b):
    return lax.dot_general(a, b, (((1,), (1,)), ((), ())), preferred_element_type=F32)


def a2a(value, axes):
    return lax.all_to_all(value, axes, 0, 0, tiled=True)


def shift(value, axis, by):
    count = lax.axis_size(axis)
    return lax.ppermute(value, axis, [(i, (i + by) % count) for i in range(count)])


def shift_x(value, by):
    pairs = []
    for p in range(2):
        for h in range(2):
            to = (h * 2 + p + by) % 4
            pairs.append((p * 2 + h, (to % 2) * 2 + to // 2))
    return lax.ppermute(value, ("p", "h"), pairs)


def silu_bf(pre):
    return jax.nn.silu(pre).astype(BF)


def slope_bf(up, pre):
    s = jax.nn.sigmoid(pre)
    return (up * s * (1.0 + pre * (1.0 - s))).astype(BF)


def cut_kernel(at_ref, x_ref, ct_ref, *outs):
    p, x, c, z, y = (at_ref[i] for i in range(5))
    tok = x_ref.shape[0]
    own = x_ref.shape[1] // 16
    half, part = tok // 2, tok // 8

    def copy(v_ref, u_ref):
        def group(i, carry):
            rc, q = i // 4, lax.rem(i, 4)
            source = lax.rem(c + rc, 2) * half + lax.rem(x + 4 - q, 4) * part
            rows = pl.ds(pl.multiple_of(source, part), part)
            to = pl.ds(pl.multiple_of(i * part, part), part)
            for k in range(4):
                for j in range(4):
                    at_v = lax.rem(z + k, 4) * 4 + lax.rem(y + 4 - j, 4)
                    at_u = lax.rem(z + 4 - j, 4) * 4 + lax.rem(y + k, 4)
                    for out, ref, at in ((outs[k], v_ref, at_v), (outs[4 + k], u_ref, at_u)):
                        cols = pl.ds(pl.multiple_of(at * own, own), own)
                        out[to, j * own : (j + 1) * own] = ref[rows, cols]
            return carry

        lax.fori_loop(0, 8, group, 0)

    @pl.when(p == 0)
    def _():
        copy(x_ref, ct_ref)

    @pl.when(p != 0)
    def _():
        copy(ct_ref, x_ref)


def cut(at, x, ct):
    tok, width = x.shape
    vmem = pl.BlockSpec(memory_space=pltpu.VMEM)
    outs = pl.pallas_call(
        cut_kernel,
        out_shape=[jax.ShapeDtypeStruct((tok, width // 4), BF)] * 8,
        in_specs=[pl.BlockSpec(memory_space=pltpu.SMEM), vmem, vmem],
        out_specs=[vmem] * 8,
        name="cut",
    )(at, x, ct)
    return list(outs[:4]), list(outs[4:])


def project_kernel(*refs):
    blocks, weights, sent, kept, left = refs[:4], refs[4:8], refs[8], refs[9], refs[10]
    tok = blocks[0].shape[0]
    half = tok // 2

    @pl.when(pl.program_id(0) == 0)
    def _():
        for k in range(4):
            left[k * half : (k + 1) * half, :] = blocks[k][half:, :]
            left[2 * tok + k * half : 2 * tok + (k + 1) * half, :] = blocks[k][:half, :]

    right = jnp.concatenate([w[...] for w in weights])
    total = dot(left[...], right)
    sent[...] = total[: 2 * tok].astype(BF)
    kept[...] = total[2 * tok :]


def project(blocks, weights):
    tok, wide = blocks[0].shape
    own, hidden = weights[0].shape
    tile = hidden // 2
    return pl.pallas_call(
        project_kernel,
        out_shape=[
            jax.ShapeDtypeStruct((2 * tok, hidden), BF),
            jax.ShapeDtypeStruct((2 * tok, hidden), F32),
        ],
        grid=(2,),
        in_specs=[pl.BlockSpec((tok, wide), lambda n: (0, 0))] * 4
        + [pl.BlockSpec((own, tile), lambda n: (0, n))] * 4,
        out_specs=[pl.BlockSpec((2 * tok, tile), lambda n: (0, n))] * 2,
        scratch_shapes=[pltpu.VMEM((4 * tok, wide), BF)],
        cost_estimate=pl.CostEstimate(
            flops=8 * tok * wide * hidden, bytes_accessed=8 * tok * wide * 2, transcendentals=0
        ),
    )(*blocks, *weights)


def turn_kernel(*refs):
    blocks, out = refs[:4], refs[4]
    tok = blocks[0].shape[0]
    half = tok // 2
    for rc in range(2):
        for k in range(4):
            to = (rc * 4 + k) * half
            out[:, to : to + half] = blocks[k][rc * half : (rc + 1) * half, :].T


def turn(blocks):
    tok, wide = blocks[0].shape
    return pl.pallas_call(
        turn_kernel,
        out_shape=jax.ShapeDtypeStruct((wide, 4 * tok), BF),
        grid=(2,),
        in_specs=[pl.BlockSpec((tok, wide // 2), lambda j: (0, j))] * 4,
        out_specs=pl.BlockSpec((wide // 2, 4 * tok), lambda j: (j, 0)),
        cost_estimate=pl.CostEstimate(
            flops=2 * tok * wide * wide, bytes_accessed=16 * tok * wide, transcendentals=0
        ),
    )(*blocks)


def split_rows(outs, total):
    own = outs[0].shape[0]
    for j in range(4):
        outs[j][...] = total[j * own : (j + 1) * own].astype(outs[j].dtype)


def grad_v_kernel(turned, *refs):
    right = jnp.concatenate([piece[...] for piece in refs[:8]])
    split_rows(refs[8:], dot(turned[...], right))


def grad_v_call(turned, pieces):
    wide, tok = turned.shape
    half, hidden = pieces[0].shape
    own, tile = wide // 4, hidden // 2
    return pl.pallas_call(
        grad_v_kernel,
        out_shape=[jax.ShapeDtypeStruct((own, hidden), t) for t in (F32, BF, BF, BF)],
        grid=(2,),
        in_specs=[pl.BlockSpec((wide, tok), lambda n: (0, 0))]
        + [pl.BlockSpec((half, tile), lambda n: (0, n))] * 8,
        out_specs=[pl.BlockSpec((own, tile), lambda n: (0, n))] * 4,
        cost_estimate=pl.CostEstimate(
            flops=2 * tok * wide * hidden, bytes_accessed=8 * tok * wide, transcendentals=0
        ),
        name="grad_v",
    )(turned, *pieces)


def grad_u_kernel(at_ref, turned, *refs):
    w_refs, pairs, outs = refs[:4], refs[4:12], refs[12:16]
    fold, factor, right, left = refs[16:]
    s = pl.program_id(0)
    own = w_refs[0].shape[0]
    half = pairs[0].shape[1]
    tile = turned.shape[1]
    first = at_ref[0] == 0

    @pl.when(s == 0)
    def _():
        for j in range(4):
            fold[j * own : (j + 1) * own, :] = w_refs[j][...]
        for i in range(8):
            act, slope = pairs[i][0], pairs[i][1]
            right[i * half : (i + 1) * half, :] = jnp.where(first, act, slope)
            factor[i * half : (i + 1) * half, :] = jnp.where(first, slope, act)

    @pl.when(s < 2)
    def _():
        at = pl.ds(pl.multiple_of(s * tile, tile), tile)
        total = turned[...].astype(F32) + dot_t1(fold[...], factor[at, :])
        left[:, at] = total.astype(BF)

    @pl.when(s >= 2)
    def _():
        width = outs[0].shape[1]
        at = pl.ds(pl.multiple_of((s - 2) * width, width), width)
        split_rows(outs, dot(left[...], right[:, at]))


def grad_u_call(at, turned, pairs, weights):
    wide, tok = turned.shape
    hidden = pairs[0].shape[2]
    own, tile = wide // 4, hidden // 2

    def late(s):
        return jnp.maximum(s - 2, 0)

    return pl.pallas_call(
        grad_u_kernel,
        out_shape=[jax.ShapeDtypeStruct((own, hidden), t) for t in (F32, BF, BF, BF)],
        grid=(4,),
        in_specs=[pl.BlockSpec(memory_space=pltpu.SMEM)]
        + [pl.BlockSpec((wide, tok // 2), lambda s: (0, jnp.minimum(s, 1)))]
        + [pl.BlockSpec((own, hidden), lambda s: (0, 0))] * 4
        + [pl.BlockSpec((2, tok // 8, hidden), lambda s: (0, 0, 0))] * 8,
        out_specs=[pl.BlockSpec((own, tile), lambda s: (0, late(s)))] * 4,
        scratch_shapes=[
            pltpu.VMEM((wide, hidden), BF),
            pltpu.VMEM((tok, hidden), BF),
            pltpu.VMEM((tok, hidden), BF),
            pltpu.VMEM((wide, tok), BF),
        ],
        cost_estimate=pl.CostEstimate(
            flops=4 * tok * wide * hidden, bytes_accessed=16 * tok * wide, transcendentals=0
        ),
        name="grad_u",
    )(at, turned, *weights, *pairs)


def join_kernel(at_ref, *refs):
    blocks, out = refs[:4], refs[4]
    z, y = at_ref[3], at_ref[4]
    part = blocks[0].shape[0] // 4
    for kz in range(4):
        for ky in range(4):
            to = (lax.rem(z + 4 - kz, 4) * 4 + lax.rem(y + 4 - ky, 4)) * part
            rows = pl.ds(pl.multiple_of(to, part), part)
            out[rows, :] = blocks[kz][ky * part : (ky + 1) * part, :]


def join(at, blocks):
    rows, hidden = blocks[0].shape
    vmem = pl.BlockSpec(memory_space=pltpu.VMEM)
    return pl.pallas_call(
        join_kernel,
        out_shape=jax.ShapeDtypeStruct((4 * rows, hidden), BF),
        in_specs=[pl.BlockSpec(memory_space=pltpu.SMEM)] + [vmem] * 4,
        out_specs=vmem,
        name="join",
    )(at, *blocks)


def gather(value, axis):
    return [value] + [shift(value, axis, k) for k in (1, 2, 3)]


def exchange(pieces, axis, sign):
    return [pieces[0]] + [shift(pieces[k], axis, sign * k) for k in (1, 2, 3)]


def sum_back(blocks, axis):
    parts = exchange([blocks[0]] + [b.astype(BF) for b in blocks[1:]], axis, -1)
    return sum((part.astype(F32) for part in parts[1:]), parts[0])


def on_device(inputs, w_in, w_out, cotangent):
    p, h, c, z, y = (lax.axis_index(a) for a in AXES)
    first = p == 0
    n_micro, rows, cols = inputs.shape
    tok = n_micro * rows
    hidden = w_in.shape[2]
    half = tok // 2
    mine = half // 4

    w_i = w_in[0]
    w_o = w_out[0].T
    w_u = jnp.where(first, w_o, w_i)
    w_v = jnp.where(first, w_i, w_o)
    w_3 = lax.ppermute(w_u, "p", [(0, 1), (1, 0)])
    w_vs = gather(w_v, "y")
    at = jnp.stack([p, h * 2 + p, c, z, y])
    vs, us = cut(at, inputs.reshape(tok, cols), cotangent.reshape(tok, cols))
    vs = exchange(vs, "z", 1)
    us = exchange(us, "y", 1)
    w_us = gather(w_u, "z")

    m = 0.0
    far_u, far_3 = shift(w_u, "c", 1), shift(w_3, "c", 1)
    for mine_u, mine_3 in ((w_u, w_3), (far_u, far_3)):
        m += dot_t0(jnp.where(first, mine_u, mine_3), jnp.where(first, mine_3, mine_u))
    m = lax.dynamic_slice(
        m.reshape(2, 16, 2, -1, hidden), (c, 0, p, 0, 0), (1, 16, 1, hidden // 64, hidden)
    )
    m = a2a(m.reshape(hidden // 4, hidden).astype(BF), ("z", "y", "h"))
    m = m.reshape(32, -1, hidden).astype(F32).sum(0).astype(BF)
    m = a2a(jnp.broadcast_to(m[None], (4,) + m.shape), ("p", "h")).reshape(-1, hidden)
    w_us[0], w_vs[0], m = lax.optimization_barrier((w_us[0], w_vs[0], m))
    m = jnp.concatenate(gather(m, "y"))
    m = gather(m, "z")
    m_near = join(at, m)
    m_far = shift(m_near, "c", 1)

    def reduced(blocks, weights, axis):
        sent, kept = project(blocks, weights)
        sent = shift(sent, "c", 1)
        kept = kept + sent.astype(F32)
        return sum_back([kept[k * half : (k + 1) * half] for k in range(4)], axis)

    a_v = reduced(vs, w_vs, "z")
    a_u = reduced(us, w_us, "y")
    w_3s = gather(w_3, "z")

    both = jnp.concatenate([a_u, a_v], 1)
    pieces = [both[(4 - k) % 4 * mine :][:mine] for k in range(4)]
    got = [pieces[0]] + [shift_x(pieces[k].astype(BF), k).astype(F32) for k in (1, 2, 3)]
    same = got[0] + got[2]
    other = got[1] + got[3]
    layer0 = jnp.where(first, same, other)
    layer1 = jnp.where(first, other, same)
    up0, pre0 = layer0[:, :hidden], layer0[:, hidden:]
    pre1, up1 = layer1[:, :hidden], layer1[:, hidden:]
    side = hidden // 2
    act0 = silu_bf(pre0)
    low, high = act0[:, :side], act0[:, side:]
    near, far = jnp.where(c == 0, low, high), jnp.where(c == 0, high, low)
    pre1 = pre1 + dot(near, m_near) + dot(far, m_far)
    act1 = silu_bf(pre1)
    slope1 = slope_bf(up1, pre1)
    near, far = dot_t1(slope1, m_near), dot_t1(slope1, m_far)
    low, high = jnp.where(c == 0, near, far), jnp.where(c == 0, far, near)
    slope0 = slope_bf(up0 + jnp.concatenate([low, high], 1), pre0)

    same = jnp.stack([jnp.where(first, slope0, act1), act0, slope1])
    other = jnp.stack([jnp.where(first, act1, slope0), act0, slope1])
    got = [same, shift_x(other, 1), shift_x(same, 2), shift_x(other, 3)]
    back = jnp.concatenate(got, 1)
    rs = gather(back[0], "z")
    pairs = gather(back[1:], "y")
    rs += [shift(a, "c", 1) for a in rs]
    pair_own = shift(pairs[0], "c", 1)
    pairs += [pair_own] + [shift(a, "c", 1) for a in pairs[1:]]

    g_v = grad_v_call(turn(vs), rs)
    g_v = sum_back(g_v, "y")
    g_u = grad_u_call(at, turn(us), pairs, w_3s)
    g_u = sum_back(g_u, "z")

    squares = jnp.sum(g_u * g_u) + jnp.sum(g_v * g_v)
    for axes, count in ((("z", "y"), 16), (("p", "h", "c"), 8)):
        row = jnp.broadcast_to(squares, (count, 8, 128))
        squares = a2a(row, axes)[:, 0, 0].sum()
    grad_norm = jnp.sqrt(squares)
    factor = jnp.minimum(1.0, CLIP_NORM / grad_norm)
    g_in = jnp.where(first, g_v, g_u) * factor
    g_out = jnp.where(first, g_u, g_v) * factor
    return (g_in[None], g_out.T[None], grad_norm)


def solution(mesh):
    split = Mesh(mesh.devices.reshape(mesh.shape["pipe"], 2, 2, 4, 4), AXES)
    tensor, dp, all_model = ("h", "c"), ("z", "y"), ("h", "c", "z", "y")
    placed = (
        P(None, dp, tensor),
        P("p", all_model, None),
        P("p", None, all_model),
        P(None, dp, tensor),
    )
    return jax.shard_map(
        on_device,
        mesh=split,
        in_specs=placed,
        out_specs=(P("p", all_model, None), P("p", None, all_model), P()),
        check_vma=False,
    )
```

```python
import jax
import jax.numpy as jnp
from jax import lax
from jax.experimental import pallas as pl
from jax.experimental.pallas import tpu as pltpu
from jax.sharding import Mesh
from jax.sharding import PartitionSpec as P


CLIP_NORM = 16384
AXES = ("p", "h", "c", "z", "y")
BF = jnp.bfloat16
F32 = jnp.float32


def dot(a, b):
    return jnp.dot(a, b, preferred_element_type=F32)


def dot_t0(a, b):
    return lax.dot_general(a, b, (((0,), (0,)), ((), ())), preferred_element_type=F32)


def dot_t1(a, b):
    return lax.dot_general(a, b, (((1,), (1,)), ((), ())), preferred_element_type=F32)


def a2a(value, axes):
    return lax.all_to_all(value, axes, 0, 0, tiled=True)


def shift(value, axis, by):
    count = lax.axis_size(axis)
    return lax.ppermute(value, axis, [(i, (i + by) % count) for i in range(count)])


def shift_x(value, by):
    pairs = []
    for p in range(2):
        for h in range(2):
            to = (h * 2 + p + by) % 4
            pairs.append((p * 2 + h, (to % 2) * 2 + to // 2))
    return lax.ppermute(value, ("p", "h"), pairs)


def silu_bf(pre):
    return jax.nn.silu(pre).astype(BF)


def slope_bf(up, pre):
    s = jax.nn.sigmoid(pre)
    return (up * s * (1.0 + pre * (1.0 - s))).astype(BF)


def cut_kernel(at_ref, x_ref, ct_ref, *outs):
    p, z, y = at_ref[0], at_ref[3], at_ref[4]
    own = x_ref.shape[1] // 16

    def copy(v_ref, u_ref):
        for k in range(4):
            for j in range(4):
                at_v = lax.rem(z + k, 4) * 4 + lax.rem(y + 4 - j, 4)
                at_u = lax.rem(z + 4 - j, 4) * 4 + lax.rem(y + k, 4)
                for out, ref, at in ((outs[k], v_ref, at_v), (outs[4 + k], u_ref, at_u)):
                    cols = pl.ds(pl.multiple_of(at * own, own), own)
                    out[:, j * own : (j + 1) * own] = ref[:, cols]

    @pl.when(p == 0)
    def _():
        copy(x_ref, ct_ref)

    @pl.when(p != 0)
    def _():
        copy(ct_ref, x_ref)


def cut(at, x, ct):
    tok, width = x.shape
    part = tok // 8

    def source(i, at_ref):
        return (lax.rem(at_ref[2] + i // 4, 2) * 4 + lax.rem(at_ref[1] + 4 - lax.rem(i, 4), 4), 0)

    outs = pl.pallas_call(
        cut_kernel,
        out_shape=[jax.ShapeDtypeStruct((tok, width // 4), BF)] * 8,
        grid_spec=pltpu.PrefetchScalarGridSpec(
            num_scalar_prefetch=1,
            grid=(8,),
            in_specs=[pl.BlockSpec((part, width), source)] * 2,
            out_specs=[pl.BlockSpec((part, width // 4), lambda i, at_ref: (i, 0))] * 8,
        ),
        name="cut",
    )(at, x, ct)
    return list(outs[:4]), list(outs[4:])


def project_kernel(*refs):
    blocks, weights, sent, kept, left = refs[:4], refs[4:8], refs[8], refs[9], refs[10]
    tok = blocks[0].shape[0]
    half = tok // 2

    @pl.when(pl.program_id(0) == 0)
    def _():
        for k in range(4):
            left[k * half : (k + 1) * half, :] = blocks[k][half:, :]
            left[2 * tok + k * half : 2 * tok + (k + 1) * half, :] = blocks[k][:half, :]

    right = jnp.concatenate([w[...] for w in weights])
    total = dot(left[...], right)
    sent[...] = total[: 2 * tok].astype(BF)
    kept[...] = total[2 * tok :]


def project(blocks, weights):
    tok, wide = blocks[0].shape
    own, hidden = weights[0].shape
    tile = hidden // 2
    return pl.pallas_call(
        project_kernel,
        out_shape=[
            jax.ShapeDtypeStruct((2 * tok, hidden), BF),
            jax.ShapeDtypeStruct((2 * tok, hidden), F32),
        ],
        grid=(2,),
        in_specs=[pl.BlockSpec((tok, wide), lambda n: (0, 0))] * 4
        + [pl.BlockSpec((own, tile), lambda n: (0, n))] * 4,
        out_specs=[pl.BlockSpec((2 * tok, tile), lambda n: (0, n))] * 2,
        scratch_shapes=[pltpu.VMEM((4 * tok, wide), BF)],
        cost_estimate=pl.CostEstimate(
            flops=8 * tok * wide * hidden, bytes_accessed=8 * tok * wide * 2, transcendentals=0
        ),
    )(*blocks, *weights)


def turn_kernel(*refs):
    blocks, out = refs[:4], refs[4]
    tok = blocks[0].shape[0]
    half = tok // 2
    for rc in range(2):
        for k in range(4):
            to = (rc * 4 + k) * half
            out[:, to : to + half] = blocks[k][rc * half : (rc + 1) * half, :].T


def turn(blocks):
    tok, wide = blocks[0].shape
    return pl.pallas_call(
        turn_kernel,
        out_shape=jax.ShapeDtypeStruct((wide, 4 * tok), BF),
        grid=(2,),
        in_specs=[pl.BlockSpec((tok, wide // 2), lambda j: (0, j))] * 4,
        out_specs=pl.BlockSpec((wide // 2, 4 * tok), lambda j: (j, 0)),
        cost_estimate=pl.CostEstimate(
            flops=2 * tok * wide * wide, bytes_accessed=16 * tok * wide, transcendentals=0
        ),
    )(*blocks)


def split_rows(outs, total):
    own = outs[0].shape[0]
    for j in range(4):
        outs[j][...] = total[j * own : (j + 1) * own].astype(outs[j].dtype)


def grad_v_kernel(turned, *refs):
    right = jnp.concatenate([piece[...] for piece in refs[:8]])
    split_rows(refs[8:], dot(turned[...], right))


def grad_v_call(turned, pieces):
    wide, tok = turned.shape
    half, hidden = pieces[0].shape
    own, tile = wide // 4, hidden // 2
    return pl.pallas_call(
        grad_v_kernel,
        out_shape=[jax.ShapeDtypeStruct((own, hidden), t) for t in (F32, BF, BF, BF)],
        grid=(2,),
        in_specs=[pl.BlockSpec((wide, tok), lambda n: (0, 0))]
        + [pl.BlockSpec((half, tile), lambda n: (0, n))] * 8,
        out_specs=[pl.BlockSpec((own, tile), lambda n: (0, n))] * 4,
        cost_estimate=pl.CostEstimate(
            flops=2 * tok * wide * hidden, bytes_accessed=8 * tok * wide, transcendentals=0
        ),
        name="grad_v",
    )(turned, *pieces)


def grad_u_kernel(at_ref, turned, *refs):
    w_refs, pairs, outs = refs[:4], refs[4:12], refs[12:16]
    fold, factor, right, left = refs[16:]
    s = pl.program_id(0)
    own = w_refs[0].shape[0]
    half = pairs[0].shape[1]
    tile = turned.shape[1]
    first = at_ref[0] == 0

    @pl.when(s == 0)
    def _():
        for j in range(4):
            fold[j * own : (j + 1) * own, :] = w_refs[j][...]
        for i in range(8):
            act, slope = pairs[i][0], pairs[i][1]
            right[i * half : (i + 1) * half, :] = jnp.where(first, act, slope)
            factor[i * half : (i + 1) * half, :] = jnp.where(first, slope, act)

    @pl.when(s < 2)
    def _():
        at = pl.ds(pl.multiple_of(s * tile, tile), tile)
        total = turned[...].astype(F32) + dot_t1(fold[...], factor[at, :])
        left[:, at] = total.astype(BF)

    @pl.when(s >= 2)
    def _():
        width = outs[0].shape[1]
        at = pl.ds(pl.multiple_of((s - 2) * width, width), width)
        split_rows(outs, dot(left[...], right[:, at]))


def grad_u_call(at, turned, pairs, weights):
    wide, tok = turned.shape
    hidden = pairs[0].shape[2]
    own, tile = wide // 4, hidden // 2

    def late(s):
        return jnp.maximum(s - 2, 0)

    return pl.pallas_call(
        grad_u_kernel,
        out_shape=[jax.ShapeDtypeStruct((own, hidden), t) for t in (F32, BF, BF, BF)],
        grid=(4,),
        in_specs=[pl.BlockSpec(memory_space=pltpu.SMEM)]
        + [pl.BlockSpec((wide, tok // 2), lambda s: (0, jnp.minimum(s, 1)))]
        + [pl.BlockSpec((own, hidden), lambda s: (0, 0))] * 4
        + [pl.BlockSpec((2, tok // 8, hidden), lambda s: (0, 0, 0))] * 8,
        out_specs=[pl.BlockSpec((own, tile), lambda s: (0, late(s)))] * 4,
        scratch_shapes=[
            pltpu.VMEM((wide, hidden), BF),
            pltpu.VMEM((tok, hidden), BF),
            pltpu.VMEM((tok, hidden), BF),
            pltpu.VMEM((wide, tok), BF),
        ],
        cost_estimate=pl.CostEstimate(
            flops=4 * tok * wide * hidden, bytes_accessed=16 * tok * wide, transcendentals=0
        ),
        name="grad_u",
    )(at, turned, *weights, *pairs)


def join_kernel(at_ref, *refs):
    blocks, out = refs[:4], refs[4]
    z, y = at_ref[3], at_ref[4]
    part = blocks[0].shape[0] // 4
    for kz in range(4):
        for ky in range(4):
            to = (lax.rem(z + 4 - kz, 4) * 4 + lax.rem(y + 4 - ky, 4)) * part
            rows = pl.ds(pl.multiple_of(to, part), part)
            out[rows, :] = blocks[kz][ky * part : (ky + 1) * part, :]


def join(at, blocks):
    rows, hidden = blocks[0].shape
    vmem = pl.BlockSpec(memory_space=pltpu.VMEM)
    return pl.pallas_call(
        join_kernel,
        out_shape=jax.ShapeDtypeStruct((4 * rows, hidden), BF),
        in_specs=[pl.BlockSpec(memory_space=pltpu.SMEM)] + [vmem] * 4,
        out_specs=vmem,
        name="join",
    )(at, *blocks)


def gather(value, axis):
    return [value] + [shift(value, axis, k) for k in (1, 2, 3)]


def exchange(pieces, axis, sign):
    return [pieces[0]] + [shift(pieces[k], axis, sign * k) for k in (1, 2, 3)]


def sum_back(blocks, axis):
    parts = exchange([blocks[0]] + [b.astype(BF) for b in blocks[1:]], axis, -1)
    return sum((part.astype(F32) for part in parts[1:]), parts[0])


def on_device(inputs, w_in, w_out, cotangent):
    p, h, c, z, y = (lax.axis_index(a) for a in AXES)
    first = p == 0
    n_micro, rows, cols = inputs.shape
    tok = n_micro * rows
    hidden = w_in.shape[2]
    half = tok // 2
    mine = half // 4

    w_i = w_in[0]
    w_o = w_out[0].T
    w_u = jnp.where(first, w_o, w_i)
    w_v = jnp.where(first, w_i, w_o)
    w_3 = lax.ppermute(w_u, "p", [(0, 1), (1, 0)])
    w_vs = gather(w_v, "y")
    at = jnp.stack([p, h * 2 + p, c, z, y])
    vs, us = cut(at, inputs.reshape(tok, cols), cotangent.reshape(tok, cols))
    vs = exchange(vs, "z", 1)
    us = exchange(us, "y", 1)
    w_us = gather(w_u, "z")

    m = 0.0
    far_u, far_3 = shift(w_u, "c", 1), shift(w_3, "c", 1)
    for mine_u, mine_3 in ((w_u, w_3), (far_u, far_3)):
        m += dot_t0(jnp.where(first, mine_u, mine_3), jnp.where(first, mine_3, mine_u))
    m = lax.dynamic_slice(
        m.reshape(2, 16, 2, -1, hidden), (c, 0, p, 0, 0), (1, 16, 1, hidden // 64, hidden)
    )
    m = a2a(m.reshape(hidden // 4, hidden).astype(BF), ("z", "y", "h"))
    m = m.reshape(32, -1, hidden).astype(F32).sum(0).astype(BF)
    m = a2a(jnp.broadcast_to(m[None], (4,) + m.shape), ("p", "h")).reshape(-1, hidden)
    w_us[0], w_vs[0], m = lax.optimization_barrier((w_us[0], w_vs[0], m))
    m = jnp.concatenate(gather(m, "y"))
    m = gather(m, "z")
    m_near = join(at, m)
    m_far = shift(m_near, "c", 1)

    def reduced(blocks, weights, axis):
        sent, kept = project(blocks, weights)
        sent = shift(sent, "c", 1)
        kept = kept + sent.astype(F32)
        return sum_back([kept[k * half : (k + 1) * half] for k in range(4)], axis)

    a_v = reduced(vs, w_vs, "z")
    a_u = reduced(us, w_us, "y")
    w_3s = gather(w_3, "z")

    both = jnp.concatenate([a_u, a_v], 1)
    pieces = [both[(4 - k) % 4 * mine :][:mine] for k in range(4)]
    got = [pieces[0]] + [shift_x(pieces[k].astype(BF), k).astype(F32) for k in (1, 2, 3)]
    same = got[0] + got[2]
    other = got[1] + got[3]
    layer0 = jnp.where(first, same, other)
    layer1 = jnp.where(first, other, same)
    up0, pre0 = layer0[:, :hidden], layer0[:, hidden:]
    pre1, up1 = layer1[:, :hidden], layer1[:, hidden:]
    side = hidden // 2
    act0 = silu_bf(pre0)
    low, high = act0[:, :side], act0[:, side:]
    near, far = jnp.where(c == 0, low, high), jnp.where(c == 0, high, low)
    pre1 = pre1 + dot(near, m_near) + dot(far, m_far)
    act1 = silu_bf(pre1)
    slope1 = slope_bf(up1, pre1)
    near, far = dot_t1(slope1, m_near), dot_t1(slope1, m_far)
    low, high = jnp.where(c == 0, near, far), jnp.where(c == 0, far, near)
    slope0 = slope_bf(up0 + jnp.concatenate([low, high], 1), pre0)

    same = jnp.stack([jnp.where(first, slope0, act1), act0, slope1])
    other = jnp.stack([jnp.where(first, act1, slope0), act0, slope1])
    got = [same, shift_x(other, 1), shift_x(same, 2), shift_x(other, 3)]
    back = jnp.concatenate(got, 1)
    rs = gather(back[0], "z")
    pairs = gather(back[1:], "y")
    rs += [shift(a, "c", 1) for a in rs]
    pair_own = shift(pairs[0], "c", 1)
    pairs += [pair_own] + [shift(a, "c", 1) for a in pairs[1:]]

    g_v = grad_v_call(turn(vs), rs)
    g_v = sum_back(g_v, "y")
    g_u = grad_u_call(at, turn(us), pairs, w_3s)
    g_u = sum_back(g_u, "z")

    squares = jnp.sum(g_u * g_u) + jnp.sum(g_v * g_v)
    row = jnp.broadcast_to(squares, (lax.axis_size(AXES), 1, 128))
    squares = a2a(row, AXES)[:, 0, 0].sum()
    grad_norm = jnp.sqrt(squares)
    factor = jnp.minimum(1.0, CLIP_NORM / grad_norm)
    g_in = jnp.where(first, g_v, g_u) * factor
    g_out = jnp.where(first, g_u, g_v) * factor
    return (g_in[None], g_out.T[None], grad_norm)


def solution(mesh):
    split = Mesh(mesh.devices.reshape(mesh.shape["pipe"], 2, 2, 4, 4), AXES)
    tensor, dp, all_model = ("h", "c"), ("z", "y"), ("h", "c", "z", "y")
    placed = (
        P(None, dp, tensor),
        P("p", all_model, None),
        P("p", None, all_model),
        P(None, dp, tensor),
    )
    return jax.shard_map(
        on_device,
        mesh=split,
        in_specs=placed,
        out_specs=(P("p", all_model, None), P("p", None, all_model), P()),
        check_vma=False,
    )
```

```python
import jax
import jax.numpy as jnp
from jax import lax
from jax.experimental import pallas as pl
from jax.experimental.pallas import tpu as pltpu
from jax.sharding import Mesh
from jax.sharding import PartitionSpec as P


CLIP_NORM = 16384
AXES = ("p", "h", "c", "z", "y")
BF = jnp.bfloat16
F32 = jnp.float32


def dot(a, b):
    return jnp.dot(a, b, preferred_element_type=F32)


def dot_t0(a, b):
    return lax.dot_general(a, b, (((0,), (0,)), ((), ())), preferred_element_type=F32)


def dot_t1(a, b):
    return lax.dot_general(a, b, (((1,), (1,)), ((), ())), preferred_element_type=F32)


def a2a(value, axes):
    return lax.all_to_all(value, axes, 0, 0, tiled=True)


def shift(value, axis, by):
    count = lax.axis_size(axis)
    return lax.ppermute(value, axis, [(i, (i + by) % count) for i in range(count)])


def shift_x(value, by):
    pairs = []
    for p in range(2):
        for h in range(2):
            to = (h * 2 + p + by) % 4
            pairs.append((p * 2 + h, (to % 2) * 2 + to // 2))
    return lax.ppermute(value, ("p", "h"), pairs)


def silu_bf(pre):
    return jax.nn.silu(pre).astype(BF)


def slope_bf(up, pre):
    s = jax.nn.sigmoid(pre)
    return (up * s * (1.0 + pre * (1.0 - s))).astype(BF)


def cut_kernel(at_ref, x_ref, ct_ref, *outs):
    p, x, c, z, y = (at_ref[i] for i in range(5))
    tok = x_ref.shape[0]
    own = x_ref.shape[1] // 16
    half, part = tok // 2, tok // 8

    def copy(v_ref, u_ref):
        def group(i, carry):
            rc, q = i // 4, lax.rem(i, 4)
            source = lax.rem(c + rc, 2) * half + lax.rem(x + 4 - q, 4) * part
            rows = pl.ds(pl.multiple_of(source, part), part)
            to = pl.ds(pl.multiple_of(i * part, part), part)
            for k in range(4):
                for j in range(4):
                    at_v = lax.rem(z + k, 4) * 4 + lax.rem(y + 4 - j, 4)
                    at_u = lax.rem(z + 4 - j, 4) * 4 + lax.rem(y + k, 4)
                    for out, ref, at in ((outs[k], v_ref, at_v), (outs[4 + k], u_ref, at_u)):
                        cols = pl.ds(pl.multiple_of(at * own, own), own)
                        out[to, j * own : (j + 1) * own] = ref[rows, cols]
            return carry

        lax.fori_loop(0, 8, group, 0)

    @pl.when(p == 0)
    def _():
        copy(x_ref, ct_ref)

    @pl.when(p != 0)
    def _():
        copy(ct_ref, x_ref)


def cut(at, x, ct):
    tok, width = x.shape
    vmem = pl.BlockSpec(memory_space=pltpu.VMEM)
    outs = pl.pallas_call(
        cut_kernel,
        out_shape=[jax.ShapeDtypeStruct((tok, width // 4), BF)] * 8,
        in_specs=[pl.BlockSpec(memory_space=pltpu.SMEM), vmem, vmem],
        out_specs=[vmem] * 8,
        name="cut",
    )(at, x, ct)
    return list(outs[:4]), list(outs[4:])


def project_kernel(*refs):
    blocks, weights, sent, kept, left = refs[:4], refs[4:8], refs[8], refs[9], refs[10]
    tok = blocks[0].shape[0]
    half = tok // 2

    @pl.when(pl.program_id(0) == 0)
    def _():
        for k in range(4):
            left[k * half : (k + 1) * half, :] = blocks[k][half:, :]
            left[2 * tok + k * half : 2 * tok + (k + 1) * half, :] = blocks[k][:half, :]

    right = jnp.concatenate([w[...] for w in weights])
    total = dot(left[...], right)
    sent[...] = total[: 2 * tok].astype(BF)
    kept[...] = total[2 * tok :]


def project(blocks, weights):
    tok, wide = blocks[0].shape
    own, hidden = weights[0].shape
    tile = hidden // 2
    return pl.pallas_call(
        project_kernel,
        out_shape=[
            jax.ShapeDtypeStruct((2 * tok, hidden), BF),
            jax.ShapeDtypeStruct((2 * tok, hidden), F32),
        ],
        grid=(2,),
        in_specs=[pl.BlockSpec((tok, wide), lambda n: (0, 0))] * 4
        + [pl.BlockSpec((own, tile), lambda n: (0, n))] * 4,
        out_specs=[pl.BlockSpec((2 * tok, tile), lambda n: (0, n))] * 2,
        scratch_shapes=[pltpu.VMEM((4 * tok, wide), BF)],
        cost_estimate=pl.CostEstimate(
            flops=8 * tok * wide * hidden, bytes_accessed=8 * tok * wide * 2, transcendentals=0
        ),
    )(*blocks, *weights)


def turn_kernel(*refs):
    blocks, out = refs[:4], refs[4]
    tok = blocks[0].shape[0]
    half = tok // 2
    for rc in range(2):
        for k in range(4):
            to = (rc * 4 + k) * half
            out[:, to : to + half] = blocks[k][rc * half : (rc + 1) * half, :].T


def turn(blocks):
    tok, wide = blocks[0].shape
    return pl.pallas_call(
        turn_kernel,
        out_shape=jax.ShapeDtypeStruct((wide, 4 * tok), BF),
        grid=(2,),
        in_specs=[pl.BlockSpec((tok, wide // 2), lambda j: (0, j))] * 4,
        out_specs=pl.BlockSpec((wide // 2, 4 * tok), lambda j: (j, 0)),
        cost_estimate=pl.CostEstimate(
            flops=2 * tok * wide * wide, bytes_accessed=16 * tok * wide, transcendentals=0
        ),
    )(*blocks)


def split_rows(outs, total):
    at = 0
    for out in outs:
        out[...] = total[at : at + out.shape[0]].astype(out.dtype)
        at += out.shape[0]


def piece_shapes(own, hidden):
    halves = [jax.ShapeDtypeStruct((own // 2, hidden), BF)] * 6
    return [jax.ShapeDtypeStruct((own, hidden), F32)] + halves


def grad_v_kernel(turned, *refs):
    right = jnp.concatenate([piece[...] for piece in refs[:8]])
    split_rows(refs[8:], dot(turned[...], right))


def grad_v_call(turned, pieces):
    wide, tok = turned.shape
    half, hidden = pieces[0].shape
    own, tile = wide // 4, hidden // 2
    return pl.pallas_call(
        grad_v_kernel,
        out_shape=piece_shapes(own, hidden),
        grid=(2,),
        in_specs=[pl.BlockSpec((wide, tok), lambda n: (0, 0))]
        + [pl.BlockSpec((half, tile), lambda n: (0, n))] * 8,
        out_specs=[pl.BlockSpec((own, tile), lambda n: (0, n))]
        + [pl.BlockSpec((own // 2, tile), lambda n: (0, n))] * 6,
        cost_estimate=pl.CostEstimate(
            flops=2 * tok * wide * hidden, bytes_accessed=8 * tok * wide, transcendentals=0
        ),
        name="grad_v",
    )(turned, *pieces)


def grad_u_kernel(at_ref, turned, *refs):
    w_refs, pairs, outs = refs[:4], refs[4:12], refs[12:19]
    fold, factor, right, left = refs[19:]
    s = pl.program_id(0)
    own = w_refs[0].shape[0]
    half = pairs[0].shape[1]
    tile = turned.shape[1]
    first = at_ref[0] == 0

    @pl.when(s == 0)
    def _():
        for j in range(4):
            fold[j * own : (j + 1) * own, :] = w_refs[j][...]
        for i in range(8):
            act, slope = pairs[i][0], pairs[i][1]
            right[i * half : (i + 1) * half, :] = jnp.where(first, act, slope)
            factor[i * half : (i + 1) * half, :] = jnp.where(first, slope, act)

    @pl.when(s < 2)
    def _():
        at = pl.ds(pl.multiple_of(s * tile, tile), tile)
        total = turned[...].astype(F32) + dot_t1(fold[...], factor[at, :])
        left[:, at] = total.astype(BF)

    @pl.when(s >= 2)
    def _():
        width = outs[0].shape[1]
        at = pl.ds(pl.multiple_of((s - 2) * width, width), width)
        split_rows(outs, dot(left[...], right[:, at]))


def grad_u_call(at, turned, pairs, weights):
    wide, tok = turned.shape
    hidden = pairs[0].shape[2]
    own, tile = wide // 4, hidden // 2

    def late(s):
        return jnp.maximum(s - 2, 0)

    return pl.pallas_call(
        grad_u_kernel,
        out_shape=piece_shapes(own, hidden),
        grid=(4,),
        in_specs=[pl.BlockSpec(memory_space=pltpu.SMEM)]
        + [pl.BlockSpec((wide, tok // 2), lambda s: (0, jnp.minimum(s, 1)))]
        + [pl.BlockSpec((own, hidden), lambda s: (0, 0))] * 4
        + [pl.BlockSpec((2, tok // 8, hidden), lambda s: (0, 0, 0))] * 8,
        out_specs=[pl.BlockSpec((own, tile), lambda s: (0, late(s)))]
        + [pl.BlockSpec((own // 2, tile), lambda s: (0, late(s)))] * 6,
        scratch_shapes=[
            pltpu.VMEM((wide, hidden), BF),
            pltpu.VMEM((tok, hidden), BF),
            pltpu.VMEM((tok, hidden), BF),
            pltpu.VMEM((wide, tok), BF),
        ],
        cost_estimate=pl.CostEstimate(
            flops=4 * tok * wide * hidden, bytes_accessed=16 * tok * wide, transcendentals=0
        ),
        name="grad_u",
    )(at, turned, *weights, *pairs)


def join_kernel(at_ref, *refs):
    blocks, out = refs[:4], refs[4]
    z, y = at_ref[3], at_ref[4]
    part = blocks[0].shape[0] // 4
    for kz in range(4):
        for ky in range(4):
            to = (lax.rem(z + 4 - kz, 4) * 4 + lax.rem(y + 4 - ky, 4)) * part
            rows = pl.ds(pl.multiple_of(to, part), part)
            out[rows, :] = blocks[kz][ky * part : (ky + 1) * part, :]


def join(at, blocks):
    rows, hidden = blocks[0].shape
    vmem = pl.BlockSpec(memory_space=pltpu.VMEM)
    return pl.pallas_call(
        join_kernel,
        out_shape=jax.ShapeDtypeStruct((4 * rows, hidden), BF),
        in_specs=[pl.BlockSpec(memory_space=pltpu.SMEM)] + [vmem] * 4,
        out_specs=vmem,
        name="join",
    )(at, *blocks)


def gather(value, axis):
    return [value] + [shift(value, axis, k) for k in (1, 2, 3)]


def exchange(pieces, axis, sign):
    return [pieces[0]] + [shift(pieces[k], axis, sign * k) for k in (1, 2, 3)]


def sum_back(blocks, axis):
    parts = exchange([blocks[0]] + [b.astype(BF) for b in blocks[1:]], axis, -1)
    return sum((part.astype(F32) for part in parts[1:]), parts[0])


def finish_kernel(own, low1, low3, high1, high3, out, squares):
    half = low1.shape[0]
    low = own[:half, :] + low1[...].astype(F32) + low3[...].astype(F32)
    high = own[half:, :] + high1[...].astype(F32) + high3[...].astype(F32)
    out[:half, :] = low
    out[half:, :] = high
    squares[0, 0] = jnp.sum(low * low + high * high)


def finish(*parts):
    vmem = pl.BlockSpec(memory_space=pltpu.VMEM)
    return pl.pallas_call(
        finish_kernel,
        out_shape=[
            jax.ShapeDtypeStruct(parts[0].shape, F32),
            jax.ShapeDtypeStruct((1, 1), F32),
        ],
        in_specs=[vmem] * 5,
        out_specs=[vmem, pl.BlockSpec(memory_space=pltpu.SMEM)],
        name="finish",
    )(*parts)


def sum_near(pieces, axis):
    own, low1, high1, low2, high2, low3, high3 = pieces
    low2, high2 = shift(low2, axis, -1), shift(high2, axis, 1)
    high1, low3 = shift(high1, axis, -1), shift(low3, axis, 1)
    low1 = (low1.astype(F32) + low2.astype(F32)).astype(BF)
    high3 = (high3.astype(F32) + high2.astype(F32)).astype(BF)
    low1, high3 = shift(low1, axis, -1), shift(high3, axis, 1)
    return finish(own, low1, low3, high1, high3)


def on_device(inputs, w_in, w_out, cotangent):
    p, h, c, z, y = (lax.axis_index(a) for a in AXES)
    first = p == 0
    n_micro, rows, cols = inputs.shape
    tok = n_micro * rows
    hidden = w_in.shape[2]
    half = tok // 2
    mine = half // 4

    w_i = w_in[0]
    w_o = w_out[0].T
    w_u = jnp.where(first, w_o, w_i)
    w_v = jnp.where(first, w_i, w_o)
    w_3 = lax.ppermute(w_u, "p", [(0, 1), (1, 0)])
    w_vs = gather(w_v, "y")
    at = jnp.stack([p, h * 2 + p, c, z, y])
    vs, us = cut(at, inputs.reshape(tok, cols), cotangent.reshape(tok, cols))
    vs = exchange(vs, "z", 1)
    us = exchange(us, "y", 1)
    w_us = gather(w_u, "z")

    m = 0.0
    far_u, far_3 = shift(w_u, "c", 1), shift(w_3, "c", 1)
    for mine_u, mine_3 in ((w_u, w_3), (far_u, far_3)):
        m += dot_t0(jnp.where(first, mine_u, mine_3), jnp.where(first, mine_3, mine_u))
    m = lax.dynamic_slice(
        m.reshape(2, 16, 2, -1, hidden), (c, 0, p, 0, 0), (1, 16, 1, hidden // 64, hidden)
    )
    m = a2a(m.reshape(hidden // 4, hidden).astype(BF), ("z", "y", "h"))
    m = m.reshape(32, -1, hidden).astype(F32).sum(0).astype(BF)
    m = a2a(jnp.broadcast_to(m[None], (4,) + m.shape), ("p", "h")).reshape(-1, hidden)
    w_us[0], w_vs[0], m = lax.optimization_barrier((w_us[0], w_vs[0], m))
    m = jnp.concatenate(gather(m, "y"))
    m = gather(m, "z")
    m_near = join(at, m)
    m_far = shift(m_near, "c", 1)

    def reduced(blocks, weights, axis):
        sent, kept = project(blocks, weights)
        sent = shift(sent, "c", 1)
        kept = kept + sent.astype(F32)
        return sum_back([kept[k * half : (k + 1) * half] for k in range(4)], axis)

    a_v = reduced(vs, w_vs, "z")
    a_u = reduced(us, w_us, "y")
    w_3s = gather(w_3, "z")

    both = jnp.concatenate([a_u, a_v], 1)
    pieces = [both[(4 - k) % 4 * mine :][:mine] for k in range(4)]
    got = [pieces[0]] + [shift_x(pieces[k].astype(BF), k).astype(F32) for k in (1, 2, 3)]
    same = got[0] + got[2]
    other = got[1] + got[3]
    layer0 = jnp.where(first, same, other)
    layer1 = jnp.where(first, other, same)
    up0, pre0 = layer0[:, :hidden], layer0[:, hidden:]
    pre1, up1 = layer1[:, :hidden], layer1[:, hidden:]
    side = hidden // 2
    act0 = silu_bf(pre0)
    low, high = act0[:, :side], act0[:, side:]
    near, far = jnp.where(c == 0, low, high), jnp.where(c == 0, high, low)
    pre1 = pre1 + dot(near, m_near) + dot(far, m_far)
    act1 = silu_bf(pre1)
    slope1 = slope_bf(up1, pre1)
    near, far = dot_t1(slope1, m_near), dot_t1(slope1, m_far)
    low, high = jnp.where(c == 0, near, far), jnp.where(c == 0, far, near)
    slope0 = slope_bf(up0 + jnp.concatenate([low, high], 1), pre0)

    same = jnp.stack([jnp.where(first, slope0, act1), act0, slope1])
    other = jnp.stack([jnp.where(first, act1, slope0), act0, slope1])
    got = [same, shift_x(other, 1), shift_x(same, 2), shift_x(other, 3)]
    back = jnp.concatenate(got, 1)
    rs = gather(back[0], "z")
    pairs = gather(back[1:], "y")
    rs += [shift(a, "c", 1) for a in rs]
    pair_own = shift(pairs[0], "c", 1)
    pairs += [pair_own] + [shift(a, "c", 1) for a in pairs[1:]]

    g_v, squares_v = sum_near(grad_v_call(turn(vs), rs), "y")
    g_u, squares_u = sum_near(grad_u_call(at, turn(us), pairs, w_3s), "z")

    squares = squares_u[0, 0] + squares_v[0, 0]
    row = jnp.broadcast_to(squares, (lax.axis_size(AXES), 1, 128))
    squares = a2a(row, AXES)[:, 0, 0].sum()
    grad_norm = jnp.sqrt(squares)
    factor = jnp.minimum(1.0, CLIP_NORM / grad_norm)
    g_in = jnp.where(first, g_v, g_u) * factor
    g_out = jnp.where(first, g_u, g_v) * factor
    return (g_in[None], g_out.T[None], grad_norm)


def solution(mesh):
    split = Mesh(mesh.devices.reshape(mesh.shape["pipe"], 2, 2, 4, 4), AXES)
    tensor, dp, all_model = ("h", "c"), ("z", "y"), ("h", "c", "z", "y")
    placed = (
        P(None, dp, tensor),
        P("p", all_model, None),
        P("p", None, all_model),
        P(None, dp, tensor),
    )
    return jax.shard_map(
        on_device,
        mesh=split,
        in_specs=placed,
        out_specs=(P("p", all_model, None), P("p", None, all_model), P()),
        check_vma=False,
    )
```

```python
import jax
import jax.numpy as jnp
from jax import lax
from jax.experimental import pallas as pl
from jax.experimental.pallas import tpu as pltpu
from jax.sharding import Mesh
from jax.sharding import PartitionSpec as P


CLIP_NORM = 16384
AXES = ("p", "h", "c", "z", "y")
BF = jnp.bfloat16
F32 = jnp.float32


def dot(a, b):
    return jnp.dot(a, b, preferred_element_type=F32)


def dot_t0(a, b):
    return lax.dot_general(a, b, (((0,), (0,)), ((), ())), preferred_element_type=F32)


def dot_t1(a, b):
    return lax.dot_general(a, b, (((1,), (1,)), ((), ())), preferred_element_type=F32)


def a2a(value, axes):
    return lax.all_to_all(value, axes, 0, 0, tiled=True)


def shift(value, axis, by):
    count = lax.axis_size(axis)
    return lax.ppermute(value, axis, [(i, (i + by) % count) for i in range(count)])


def shift_x(value, by):
    pairs = []
    for p in range(2):
        for h in range(2):
            to = (h * 2 + p + by) % 4
            pairs.append((p * 2 + h, (to % 2) * 2 + to // 2))
    return lax.ppermute(value, ("p", "h"), pairs)


def silu_bf(pre):
    return jax.nn.silu(pre).astype(BF)


def slope_bf(up, pre):
    s = jax.nn.sigmoid(pre)
    return (up * s * (1.0 + pre * (1.0 - s))).astype(BF)


def cut_kernel(at_ref, x_ref, ct_ref, *outs):
    p, x, c, z, y = (at_ref[i] for i in range(5))
    tok = x_ref.shape[0]
    own = x_ref.shape[1] // 16
    half, part = tok // 2, tok // 8

    def copy(v_ref, u_ref):
        def group(i, carry):
            rc, q = i // 4, lax.rem(i, 4)
            source = lax.rem(c + rc, 2) * half + lax.rem(x + 4 - q, 4) * part
            rows = pl.ds(pl.multiple_of(source, part), part)
            to = pl.ds(pl.multiple_of(i * part, part), part)
            for k in range(4):
                for j in range(4):
                    at_v = lax.rem(z + k, 4) * 4 + lax.rem(y + 4 - j, 4)
                    at_u = lax.rem(z + 4 - j, 4) * 4 + lax.rem(y + k, 4)
                    for out, ref, at in ((outs[k], v_ref, at_v), (outs[4 + k], u_ref, at_u)):
                        cols = pl.ds(pl.multiple_of(at * own, own), own)
                        out[to, j * own : (j + 1) * own] = ref[rows, cols]
            return carry

        lax.fori_loop(0, 8, group, 0)

    @pl.when(p == 0)
    def _():
        copy(x_ref, ct_ref)

    @pl.when(p != 0)
    def _():
        copy(ct_ref, x_ref)


def cut(at, x, ct):
    tok, width = x.shape
    vmem = pl.BlockSpec(memory_space=pltpu.VMEM)
    outs = pl.pallas_call(
        cut_kernel,
        out_shape=[jax.ShapeDtypeStruct((tok, width // 4), BF)] * 8,
        in_specs=[pl.BlockSpec(memory_space=pltpu.SMEM), vmem, vmem],
        out_specs=[vmem] * 8,
        name="cut",
    )(at, x, ct)
    return list(outs[:4]), list(outs[4:])


def project_kernel(*refs):
    blocks, weights, sent, kept, left = refs[:4], refs[4:8], refs[8], refs[9], refs[10]
    tok = blocks[0].shape[0]
    half = tok // 2

    @pl.when(pl.program_id(0) == 0)
    def _():
        for k in range(4):
            left[k * half : (k + 1) * half, :] = blocks[k][half:, :]
            left[2 * tok + k * half : 2 * tok + (k + 1) * half, :] = blocks[k][:half, :]

    right = jnp.concatenate([w[...] for w in weights])
    total = dot(left[...], right)
    sent[...] = total[: 2 * tok].astype(BF)
    kept[...] = total[2 * tok :]


def project(blocks, weights):
    tok, wide = blocks[0].shape
    own, hidden = weights[0].shape
    tile = hidden // 2
    return pl.pallas_call(
        project_kernel,
        out_shape=[
            jax.ShapeDtypeStruct((2 * tok, hidden), BF),
            jax.ShapeDtypeStruct((2 * tok, hidden), F32),
        ],
        grid=(2,),
        in_specs=[pl.BlockSpec((tok, wide), lambda n: (0, 0))] * 4
        + [pl.BlockSpec((own, tile), lambda n: (0, n))] * 4,
        out_specs=[pl.BlockSpec((2 * tok, tile), lambda n: (0, n))] * 2,
        scratch_shapes=[pltpu.VMEM((4 * tok, wide), BF)],
        cost_estimate=pl.CostEstimate(
            flops=8 * tok * wide * hidden, bytes_accessed=8 * tok * wide * 2, transcendentals=0
        ),
    )(*blocks, *weights)


def turn_kernel(*refs):
    blocks, out = refs[:4], refs[4]
    tok = blocks[0].shape[0]
    half = tok // 2
    for rc in range(2):
        for k in range(4):
            to = (rc * 4 + k) * half
            out[:, to : to + half] = blocks[k][rc * half : (rc + 1) * half, :].T


def turn(blocks):
    tok, wide = blocks[0].shape
    return pl.pallas_call(
        turn_kernel,
        out_shape=jax.ShapeDtypeStruct((wide, 4 * tok), BF),
        grid=(2,),
        in_specs=[pl.BlockSpec((tok, wide // 2), lambda j: (0, j))] * 4,
        out_specs=pl.BlockSpec((wide // 2, 4 * tok), lambda j: (j, 0)),
        cost_estimate=pl.CostEstimate(
            flops=2 * tok * wide * wide, bytes_accessed=16 * tok * wide, transcendentals=0
        ),
    )(*blocks)


def split_rows(outs, total):
    at = 0
    for out in outs:
        out[...] = total[at : at + out.shape[0]].astype(out.dtype)
        at += out.shape[0]


def piece_shapes(own, hidden):
    halves = [jax.ShapeDtypeStruct((own // 2, hidden), BF)] * 6
    return [jax.ShapeDtypeStruct((own, hidden), F32)] + halves


def grad_v_kernel(turned, *refs):
    right = jnp.concatenate([piece[...] for piece in refs[:8]])
    split_rows(refs[8:], dot(turned[...], right))


def grad_v_call(turned, pieces):
    wide, tok = turned.shape
    half, hidden = pieces[0].shape
    own, tile = wide // 4, hidden // 2
    return pl.pallas_call(
        grad_v_kernel,
        out_shape=[jax.ShapeDtypeStruct((own, hidden), t) for t in (F32, BF, BF, BF)],
        grid=(2,),
        in_specs=[pl.BlockSpec((wide, tok), lambda n: (0, 0))]
        + [pl.BlockSpec((half, tile), lambda n: (0, n))] * 8,
        out_specs=[pl.BlockSpec((own, tile), lambda n: (0, n))] * 4,
        cost_estimate=pl.CostEstimate(
            flops=2 * tok * wide * hidden, bytes_accessed=8 * tok * wide, transcendentals=0
        ),
        name="grad_v",
    )(turned, *pieces)


def grad_u_kernel(at_ref, turned, *refs):
    w_refs, pairs, outs = refs[:4], refs[4:12], refs[12:19]
    fold, factor, right, left = refs[19:]
    s = pl.program_id(0)
    own = w_refs[0].shape[0]
    half = pairs[0].shape[1]
    tile = turned.shape[1]
    first = at_ref[0] == 0

    @pl.when(s == 0)
    def _():
        for j in range(4):
            fold[j * own : (j + 1) * own, :] = w_refs[j][...]
        for i in range(8):
            act, slope = pairs[i][0], pairs[i][1]
            right[i * half : (i + 1) * half, :] = jnp.where(first, act, slope)
            factor[i * half : (i + 1) * half, :] = jnp.where(first, slope, act)

    @pl.when(s < 2)
    def _():
        at = pl.ds(pl.multiple_of(s * tile, tile), tile)
        total = turned[...].astype(F32) + dot_t1(fold[...], factor[at, :])
        left[:, at] = total.astype(BF)

    @pl.when(s >= 2)
    def _():
        width = outs[0].shape[1]
        at = pl.ds(pl.multiple_of((s - 2) * width, width), width)
        split_rows(outs, dot(left[...], right[:, at]))


def grad_u_call(at, turned, pairs, weights):
    wide, tok = turned.shape
    hidden = pairs[0].shape[2]
    own, tile = wide // 4, hidden // 2

    def late(s):
        return jnp.maximum(s - 2, 0)

    return pl.pallas_call(
        grad_u_kernel,
        out_shape=piece_shapes(own, hidden),
        grid=(4,),
        in_specs=[pl.BlockSpec(memory_space=pltpu.SMEM)]
        + [pl.BlockSpec((wide, tok // 2), lambda s: (0, jnp.minimum(s, 1)))]
        + [pl.BlockSpec((own, hidden), lambda s: (0, 0))] * 4
        + [pl.BlockSpec((2, tok // 8, hidden), lambda s: (0, 0, 0))] * 8,
        out_specs=[pl.BlockSpec((own, tile), lambda s: (0, late(s)))]
        + [pl.BlockSpec((own // 2, tile), lambda s: (0, late(s)))] * 6,
        scratch_shapes=[
            pltpu.VMEM((wide, hidden), BF),
            pltpu.VMEM((tok, hidden), BF),
            pltpu.VMEM((tok, hidden), BF),
            pltpu.VMEM((wide, tok), BF),
        ],
        cost_estimate=pl.CostEstimate(
            flops=4 * tok * wide * hidden, bytes_accessed=16 * tok * wide, transcendentals=0
        ),
        name="grad_u",
    )(at, turned, *weights, *pairs)


def join_kernel(at_ref, *refs):
    blocks, out = refs[:4], refs[4]
    z, y = at_ref[3], at_ref[4]
    part = blocks[0].shape[0] // 4
    for kz in range(4):
        for ky in range(4):
            to = (lax.rem(z + 4 - kz, 4) * 4 + lax.rem(y + 4 - ky, 4)) * part
            rows = pl.ds(pl.multiple_of(to, part), part)
            out[rows, :] = blocks[kz][ky * part : (ky + 1) * part, :]


def join(at, blocks):
    rows, hidden = blocks[0].shape
    vmem = pl.BlockSpec(memory_space=pltpu.VMEM)
    return pl.pallas_call(
        join_kernel,
        out_shape=jax.ShapeDtypeStruct((4 * rows, hidden), BF),
        in_specs=[pl.BlockSpec(memory_space=pltpu.SMEM)] + [vmem] * 4,
        out_specs=vmem,
        name="join",
    )(at, *blocks)


def gather(value, axis):
    return [value] + [shift(value, axis, k) for k in (1, 2, 3)]


def exchange(pieces, axis, sign):
    return [pieces[0]] + [shift(pieces[k], axis, sign * k) for k in (1, 2, 3)]


def sum_back(blocks, axis):
    parts = exchange([blocks[0]] + [b.astype(BF) for b in blocks[1:]], axis, -1)
    return sum((part.astype(F32) for part in parts[1:]), parts[0])


def sum_near(pieces, axis):
    own, low1, high1, low2, high2, low3, high3 = pieces
    low2, high2 = shift(low2, axis, -1), shift(high2, axis, 1)
    high1, low3 = shift(high1, axis, -1), shift(low3, axis, 1)
    low1 = (low1.astype(F32) + low2.astype(F32)).astype(BF)
    high3 = (high3.astype(F32) + high2.astype(F32)).astype(BF)
    low1, high3 = shift(low1, axis, -1), shift(high3, axis, 1)
    one = jnp.concatenate([low1, high1]).astype(F32)
    three = jnp.concatenate([low3, high3]).astype(F32)
    return own + one + three


def on_device(inputs, w_in, w_out, cotangent):
    p, h, c, z, y = (lax.axis_index(a) for a in AXES)
    first = p == 0
    n_micro, rows, cols = inputs.shape
    tok = n_micro * rows
    hidden = w_in.shape[2]
    half = tok // 2
    mine = half // 4

    w_i = w_in[0]
    w_o = w_out[0].T
    w_u = jnp.where(first, w_o, w_i)
    w_v = jnp.where(first, w_i, w_o)
    w_3 = lax.ppermute(w_u, "p", [(0, 1), (1, 0)])
    w_vs = gather(w_v, "y")
    at = jnp.stack([p, h * 2 + p, c, z, y])
    vs, us = cut(at, inputs.reshape(tok, cols), cotangent.reshape(tok, cols))
    vs = exchange(vs, "z", 1)
    us = exchange(us, "y", 1)
    w_us = gather(w_u, "z")

    m = 0.0
    far_u, far_3 = shift(w_u, "c", 1), shift(w_3, "c", 1)
    for mine_u, mine_3 in ((w_u, w_3), (far_u, far_3)):
        m += dot_t0(jnp.where(first, mine_u, mine_3), jnp.where(first, mine_3, mine_u))
    m = lax.dynamic_slice(
        m.reshape(2, 16, 2, -1, hidden), (c, 0, p, 0, 0), (1, 16, 1, hidden // 64, hidden)
    )
    m = a2a(m.reshape(hidden // 4, hidden).astype(BF), ("z", "y", "h"))
    m = m.reshape(32, -1, hidden).astype(F32).sum(0).astype(BF)
    m = a2a(jnp.broadcast_to(m[None], (4,) + m.shape), ("p", "h")).reshape(-1, hidden)
    w_us[0], w_vs[0], m = lax.optimization_barrier((w_us[0], w_vs[0], m))
    m = jnp.concatenate(gather(m, "y"))
    m = gather(m, "z")
    m_near = join(at, m)
    m_far = shift(m_near, "c", 1)

    def reduced(blocks, weights, axis):
        sent, kept = project(blocks, weights)
        sent = shift(sent, "c", 1)
        kept = kept + sent.astype(F32)
        return sum_back([kept[k * half : (k + 1) * half] for k in range(4)], axis)

    a_v = reduced(vs, w_vs, "z")
    a_u = reduced(us, w_us, "y")
    w_3s = gather(w_3, "z")

    both = jnp.concatenate([a_u, a_v], 1)
    pieces = [both[(4 - k) % 4 * mine :][:mine] for k in range(4)]
    got = [pieces[0]] + [shift_x(pieces[k].astype(BF), k).astype(F32) for k in (1, 2, 3)]
    same = got[0] + got[2]
    other = got[1] + got[3]
    layer0 = jnp.where(first, same, other)
    layer1 = jnp.where(first, other, same)
    up0, pre0 = layer0[:, :hidden], layer0[:, hidden:]
    pre1, up1 = layer1[:, :hidden], layer1[:, hidden:]
    side = hidden // 2
    act0 = silu_bf(pre0)
    low, high = act0[:, :side], act0[:, side:]
    near, far = jnp.where(c == 0, low, high), jnp.where(c == 0, high, low)
    pre1 = pre1 + dot(near, m_near) + dot(far, m_far)
    act1 = silu_bf(pre1)
    slope1 = slope_bf(up1, pre1)
    near, far = dot_t1(slope1, m_near), dot_t1(slope1, m_far)
    low, high = jnp.where(c == 0, near, far), jnp.where(c == 0, far, near)
    slope0 = slope_bf(up0 + jnp.concatenate([low, high], 1), pre0)

    same = jnp.stack([jnp.where(first, slope0, act1), act0, slope1])
    other = jnp.stack([jnp.where(first, act1, slope0), act0, slope1])
    got = [same, shift_x(other, 1), shift_x(same, 2), shift_x(other, 3)]
    back = jnp.concatenate(got, 1)
    rs = gather(back[0], "z")
    pairs = gather(back[1:], "y")
    rs += [shift(a, "c", 1) for a in rs]
    pair_own = shift(pairs[0], "c", 1)
    pairs += [pair_own] + [shift(a, "c", 1) for a in pairs[1:]]

    g_v = grad_v_call(turn(vs), rs)
    g_v = sum_back(g_v, "y")
    g_u = sum_near(grad_u_call(at, turn(us), pairs, w_3s), "z")

    squares = jnp.sum(g_u * g_u) + jnp.sum(g_v * g_v)
    row = jnp.broadcast_to(squares, (lax.axis_size(AXES), 1, 128))
    squares = a2a(row, AXES)[:, 0, 0].sum()
    grad_norm = jnp.sqrt(squares)
    factor = jnp.minimum(1.0, CLIP_NORM / grad_norm)
    g_in = jnp.where(first, g_v, g_u) * factor
    g_out = jnp.where(first, g_u, g_v) * factor
    return (g_in[None], g_out.T[None], grad_norm)


def solution(mesh):
    split = Mesh(mesh.devices.reshape(mesh.shape["pipe"], 2, 2, 4, 4), AXES)
    tensor, dp, all_model = ("h", "c"), ("z", "y"), ("h", "c", "z", "y")
    placed = (
        P(None, dp, tensor),
        P("p", all_model, None),
        P("p", None, all_model),
        P(None, dp, tensor),
    )
    return jax.shard_map(
        on_device,
        mesh=split,
        in_specs=placed,
        out_specs=(P("p", all_model, None), P("p", None, all_model), P()),
        check_vma=False,
    )
```

```python
import jax
import jax.numpy as jnp
from jax import lax
from jax.experimental import pallas as pl
from jax.experimental.pallas import tpu as pltpu
from jax.sharding import Mesh
from jax.sharding import PartitionSpec as P


CLIP_NORM = 16384
AXES = ("p", "h", "c", "z", "y")
BF = jnp.bfloat16
F32 = jnp.float32


def dot(a, b):
    return jnp.dot(a, b, preferred_element_type=F32)


def dot_t0(a, b):
    return lax.dot_general(a, b, (((0,), (0,)), ((), ())), preferred_element_type=F32)


def dot_t1(a, b):
    return lax.dot_general(a, b, (((1,), (1,)), ((), ())), preferred_element_type=F32)


def a2a(value, axes):
    return lax.all_to_all(value, axes, 0, 0, tiled=True)


def shift(value, axis, by):
    count = lax.axis_size(axis)
    return lax.ppermute(value, axis, [(i, (i + by) % count) for i in range(count)])


def shift_x(value, by):
    pairs = []
    for p in range(2):
        for h in range(2):
            to = (h * 2 + p + by) % 4
            pairs.append((p * 2 + h, (to % 2) * 2 + to // 2))
    return lax.ppermute(value, ("p", "h"), pairs)


def silu_bf(pre):
    return jax.nn.silu(pre).astype(BF)


def slope_bf(up, pre):
    s = jax.nn.sigmoid(pre)
    return (up * s * (1.0 + pre * (1.0 - s))).astype(BF)


def cut_kernel(at_ref, x_ref, ct_ref, *outs):
    p, x, c, z, y = (at_ref[i] for i in range(5))
    tok = x_ref.shape[0]
    own = x_ref.shape[1] // 16
    half, part = tok // 2, tok // 8

    def copy(v_ref, u_ref):
        def group(i, carry):
            rc, q = i // 4, lax.rem(i, 4)
            source = lax.rem(c + rc, 2) * half + lax.rem(x + 4 - q, 4) * part
            rows = pl.ds(pl.multiple_of(source, part), part)
            to = pl.ds(pl.multiple_of(i * part, part), part)
            for k in range(4):
                for j in range(4):
                    at_v = lax.rem(z + k, 4) * 4 + lax.rem(y + 4 - j, 4)
                    at_u = lax.rem(z + 4 - j, 4) * 4 + lax.rem(y + k, 4)
                    for out, ref, at in ((outs[k], v_ref, at_v), (outs[4 + k], u_ref, at_u)):
                        cols = pl.ds(pl.multiple_of(at * own, own), own)
                        out[to, j * own : (j + 1) * own] = ref[rows, cols]
            return carry

        lax.fori_loop(0, 8, group, 0)

    @pl.when(p == 0)
    def _():
        copy(x_ref, ct_ref)

    @pl.when(p != 0)
    def _():
        copy(ct_ref, x_ref)


def cut(at, x, ct):
    tok, width = x.shape
    vmem = pl.BlockSpec(memory_space=pltpu.VMEM)
    outs = pl.pallas_call(
        cut_kernel,
        out_shape=[jax.ShapeDtypeStruct((tok, width // 4), BF)] * 8,
        in_specs=[pl.BlockSpec(memory_space=pltpu.SMEM), vmem, vmem],
        out_specs=[vmem] * 8,
        name="cut",
    )(at, x, ct)
    return list(outs[:4]), list(outs[4:])


def project_kernel(*refs):
    blocks, weights, sent, kept, left = refs[:4], refs[4:8], refs[8], refs[9], refs[10]
    tok = blocks[0].shape[0]
    half = tok // 2

    @pl.when(pl.program_id(0) == 0)
    def _():
        for k in range(4):
            left[k * half : (k + 1) * half, :] = blocks[k][half:, :]
            left[2 * tok + k * half : 2 * tok + (k + 1) * half, :] = blocks[k][:half, :]

    right = jnp.concatenate([w[...] for w in weights])
    total = dot(left[...], right)
    sent[...] = total[: 2 * tok].astype(BF)
    kept[...] = total[2 * tok :]


def project(blocks, weights):
    tok, wide = blocks[0].shape
    own, hidden = weights[0].shape
    tile = hidden // 2
    return pl.pallas_call(
        project_kernel,
        out_shape=[
            jax.ShapeDtypeStruct((2 * tok, hidden), BF),
            jax.ShapeDtypeStruct((2 * tok, hidden), F32),
        ],
        grid=(2,),
        in_specs=[pl.BlockSpec((tok, wide), lambda n: (0, 0))] * 4
        + [pl.BlockSpec((own, tile), lambda n: (0, n))] * 4,
        out_specs=[pl.BlockSpec((2 * tok, tile), lambda n: (0, n))] * 2,
        scratch_shapes=[pltpu.VMEM((4 * tok, wide), BF)],
        cost_estimate=pl.CostEstimate(
            flops=8 * tok * wide * hidden, bytes_accessed=8 * tok * wide * 2, transcendentals=0
        ),
    )(*blocks, *weights)


def turn_kernel(*refs):
    blocks, out = refs[:4], refs[4]
    tok = blocks[0].shape[0]
    half = tok // 2
    for rc in range(2):
        for k in range(4):
            to = (rc * 4 + k) * half
            out[:, to : to + half] = blocks[k][rc * half : (rc + 1) * half, :].T


def turn(blocks):
    tok, wide = blocks[0].shape
    return pl.pallas_call(
        turn_kernel,
        out_shape=jax.ShapeDtypeStruct((wide, 4 * tok), BF),
        grid=(2,),
        in_specs=[pl.BlockSpec((tok, wide // 2), lambda j: (0, j))] * 4,
        out_specs=pl.BlockSpec((wide // 2, 4 * tok), lambda j: (j, 0)),
        cost_estimate=pl.CostEstimate(
            flops=2 * tok * wide * wide, bytes_accessed=16 * tok * wide, transcendentals=0
        ),
    )(*blocks)


def split_rows(outs, total):
    at = 0
    for out in outs:
        out[...] = total[at : at + out.shape[0]].astype(out.dtype)
        at += out.shape[0]


def piece_shapes(own, hidden):
    halves = [jax.ShapeDtypeStruct((own // 2, hidden), BF)] * 6
    return [jax.ShapeDtypeStruct((own, hidden), F32)] + halves


def grad_v_kernel(turned, *refs):
    right = jnp.concatenate([piece[...] for piece in refs[:8]])
    split_rows(refs[8:], dot(turned[...], right))


def grad_v_call(turned, pieces):
    wide, tok = turned.shape
    half, hidden = pieces[0].shape
    own, tile = wide // 4, hidden // 2
    return pl.pallas_call(
        grad_v_kernel,
        out_shape=[jax.ShapeDtypeStruct((own, hidden), t) for t in (F32, BF, BF, BF)],
        grid=(2,),
        in_specs=[pl.BlockSpec((wide, tok), lambda n: (0, 0))]
        + [pl.BlockSpec((half, tile), lambda n: (0, n))] * 8,
        out_specs=[pl.BlockSpec((own, tile), lambda n: (0, n))] * 4,
        cost_estimate=pl.CostEstimate(
            flops=2 * tok * wide * hidden, bytes_accessed=8 * tok * wide, transcendentals=0
        ),
        name="grad_v",
    )(turned, *pieces)


def grad_u_kernel(at_ref, turned, *refs):
    w_refs, pairs, outs = refs[:4], refs[4:12], refs[12:19]
    fold, factor, right, left = refs[19:]
    s = pl.program_id(0)
    own = w_refs[0].shape[0]
    half = pairs[0].shape[1]
    tile = turned.shape[1]
    first = at_ref[0] == 0

    @pl.when(s == 0)
    def _():
        for j in range(4):
            fold[j * own : (j + 1) * own, :] = w_refs[j][...]
        for i in range(8):
            act, slope = pairs[i][0], pairs[i][1]
            right[i * half : (i + 1) * half, :] = jnp.where(first, act, slope)
            factor[i * half : (i + 1) * half, :] = jnp.where(first, slope, act)

    @pl.when(s < 2)
    def _():
        at = pl.ds(pl.multiple_of(s * tile, tile), tile)
        total = turned[...].astype(F32) + dot_t1(fold[...], factor[at, :])
        left[:, at] = total.astype(BF)

    @pl.when(s >= 2)
    def _():
        width = outs[0].shape[1]
        at = pl.ds(pl.multiple_of((s - 2) * width, width), width)
        split_rows(outs, dot(left[...], right[:, at]))


def grad_u_call(at, turned, pairs, weights):
    wide, tok = turned.shape
    hidden = pairs[0].shape[2]
    own, tile = wide // 4, hidden // 2

    def late(s):
        return jnp.maximum(s - 2, 0)

    return pl.pallas_call(
        grad_u_kernel,
        out_shape=piece_shapes(own, hidden),
        grid=(4,),
        in_specs=[pl.BlockSpec(memory_space=pltpu.SMEM)]
        + [pl.BlockSpec((wide, tok // 2), lambda s: (0, jnp.minimum(s, 1)))]
        + [pl.BlockSpec((own, hidden), lambda s: (0, 0))] * 4
        + [pl.BlockSpec((2, tok // 8, hidden), lambda s: (0, 0, 0))] * 8,
        out_specs=[pl.BlockSpec((own, tile), lambda s: (0, late(s)))]
        + [pl.BlockSpec((own // 2, tile), lambda s: (0, late(s)))] * 6,
        scratch_shapes=[
            pltpu.VMEM((wide, hidden), BF),
            pltpu.VMEM((tok, hidden), BF),
            pltpu.VMEM((tok, hidden), BF),
            pltpu.VMEM((wide, tok), BF),
        ],
        cost_estimate=pl.CostEstimate(
            flops=4 * tok * wide * hidden, bytes_accessed=16 * tok * wide, transcendentals=0
        ),
        name="grad_u",
    )(at, turned, *weights, *pairs)


def join_kernel(at_ref, *refs):
    blocks, out = refs[:4], refs[4]
    z, y = at_ref[3], at_ref[4]
    part = blocks[0].shape[0] // 4
    for kz in range(4):
        for ky in range(4):
            to = (lax.rem(z + 4 - kz, 4) * 4 + lax.rem(y + 4 - ky, 4)) * part
            rows = pl.ds(pl.multiple_of(to, part), part)
            out[rows, :] = blocks[kz][ky * part : (ky + 1) * part, :]


def join(at, blocks):
    rows, hidden = blocks[0].shape
    vmem = pl.BlockSpec(memory_space=pltpu.VMEM)
    return pl.pallas_call(
        join_kernel,
        out_shape=jax.ShapeDtypeStruct((4 * rows, hidden), BF),
        in_specs=[pl.BlockSpec(memory_space=pltpu.SMEM)] + [vmem] * 4,
        out_specs=vmem,
        name="join",
    )(at, *blocks)


def gather(value, axis):
    return [value] + [shift(value, axis, k) for k in (1, 2, 3)]


def exchange(pieces, axis, sign):
    return [pieces[0]] + [shift(pieces[k], axis, sign * k) for k in (1, 2, 3)]


def sum_back(blocks, axis):
    parts = exchange([blocks[0]] + [b.astype(BF) for b in blocks[1:]], axis, -1)
    return sum((part.astype(F32) for part in parts[1:]), parts[0])


def sum_near(pieces, axis):
    own, low1, high1, low2, high2, low3, high3 = pieces
    low2, high2 = shift(low2, axis, -1), shift(high2, axis, 1)
    high1, low3 = shift(high1, axis, -1), shift(low3, axis, 1)
    low1 = (low1.astype(F32) + low2.astype(F32)).astype(BF)
    high3 = (high3.astype(F32) + high2.astype(F32)).astype(BF)
    low1, high3 = shift(low1, axis, -1), shift(high3, axis, 1)
    one = jnp.concatenate([low1, high1]).astype(F32)
    three = jnp.concatenate([low3, high3]).astype(F32)
    return own + one + three


def on_device(inputs, w_in, w_out, cotangent):
    p, h, c, z, y = (lax.axis_index(a) for a in AXES)
    first = p == 0
    n_micro, rows, cols = inputs.shape
    tok = n_micro * rows
    hidden = w_in.shape[2]
    half = tok // 2
    mine = half // 4

    w_i = w_in[0]
    w_o = w_out[0].T
    w_u = jnp.where(first, w_o, w_i)
    w_v = jnp.where(first, w_i, w_o)
    w_3 = lax.ppermute(w_u, "p", [(0, 1), (1, 0)])
    w_vs = gather(w_v, "y")
    at = jnp.stack([p, h * 2 + p, c, z, y])
    vs, us = cut(at, inputs.reshape(tok, cols), cotangent.reshape(tok, cols))
    vs = exchange(vs, "z", 1)
    us = exchange(us, "y", 1)
    w_us = gather(w_u, "z")

    m = 0.0
    far_u, far_3 = shift(w_u, "c", 1), shift(w_3, "c", 1)
    for mine_u, mine_3 in ((w_u, w_3), (far_u, far_3)):
        m += dot_t0(jnp.where(first, mine_u, mine_3), jnp.where(first, mine_3, mine_u))
    m = lax.dynamic_slice(
        m.reshape(2, 16, 2, -1, hidden), (c, 0, p, 0, 0), (1, 16, 1, hidden // 64, hidden)
    )
    m = a2a(m.reshape(hidden // 4, hidden).astype(BF), ("z", "y", "h"))
    m = m.reshape(32, -1, hidden).astype(F32).sum(0).astype(BF)
    m = a2a(jnp.broadcast_to(m[None], (4,) + m.shape), ("p", "h")).reshape(-1, hidden)
    w_us[0], w_vs[0], m = lax.optimization_barrier((w_us[0], w_vs[0], m))
    m = jnp.concatenate(gather(m, "y"))
    m = gather(m, "z")
    m_near = join(at, m)
    m_far = shift(m_near, "c", 1)

    def reduced(blocks, weights, axis):
        sent, kept = project(blocks, weights)
        sent = shift(sent, "c", 1)
        kept = kept + sent.astype(F32)
        return sum_back([kept[k * half : (k + 1) * half] for k in range(4)], axis)

    a_v = reduced(vs, w_vs, "z")
    a_u = reduced(us, w_us, "y")
    w_3s = gather(w_3, "z")

    both = jnp.concatenate([a_u, a_v], 1)
    pieces = [both[(4 - k) % 4 * mine :][:mine] for k in range(4)]
    got = [pieces[0]] + [shift_x(pieces[k].astype(BF), k).astype(F32) for k in (1, 2, 3)]
    same = got[0] + got[2]
    other = got[1] + got[3]
    layer0 = jnp.where(first, same, other)
    layer1 = jnp.where(first, other, same)
    up0, pre0 = layer0[:, :hidden], layer0[:, hidden:]
    pre1, up1 = layer1[:, :hidden], layer1[:, hidden:]
    side = hidden // 2
    act0 = silu_bf(pre0)
    low, high = act0[:, :side], act0[:, side:]
    near, far = jnp.where(c == 0, low, high), jnp.where(c == 0, high, low)
    pre1 = pre1 + dot(near, m_near) + dot(far, m_far)
    act1 = silu_bf(pre1)
    slope1 = slope_bf(up1, pre1)
    near, far = dot_t1(slope1, m_near), dot_t1(slope1, m_far)
    low, high = jnp.where(c == 0, near, far), jnp.where(c == 0, far, near)
    slope0 = slope_bf(up0 + jnp.concatenate([low, high], 1), pre0)

    same = jnp.stack([jnp.where(first, slope0, act1), act0, slope1])
    other = jnp.stack([jnp.where(first, act1, slope0), act0, slope1])
    got = [same, shift_x(other, 1), shift_x(same, 2), shift_x(other, 3)]
    back = jnp.concatenate(got, 1)
    rs, pairs = [back[0]], [back[1:]]
    for k in (1, 2, 3):
        rs.append(shift(rs[0], "z", k))
        pairs.append(shift(pairs[0], "y", k))
    rs += [shift(a, "c", 1) for a in rs]
    pair_own = shift(pairs[0], "c", 1)
    pairs += [pair_own] + [shift(a, "c", 1) for a in pairs[1:]]

    g_v = grad_v_call(turn(vs), rs)
    g_v = sum_back(g_v, "y")
    g_u = sum_near(grad_u_call(at, turn(us), pairs, w_3s), "z")

    squares = jnp.sum(g_u * g_u) + jnp.sum(g_v * g_v)
    row = jnp.broadcast_to(squares, (lax.axis_size(AXES), 1, 128))
    squares = a2a(row, AXES)[:, 0, 0].sum()
    grad_norm = jnp.sqrt(squares)
    factor = jnp.minimum(1.0, CLIP_NORM / grad_norm)
    g_in = jnp.where(first, g_v, g_u) * factor
    g_out = jnp.where(first, g_u, g_v) * factor
    return (g_in[None], g_out.T[None], grad_norm)


def solution(mesh):
    split = Mesh(mesh.devices.reshape(mesh.shape["pipe"], 2, 2, 4, 4), AXES)
    tensor, dp, all_model = ("h", "c"), ("z", "y"), ("h", "c", "z", "y")
    placed = (
        P(None, dp, tensor),
        P("p", all_model, None),
        P("p", None, all_model),
        P(None, dp, tensor),
    )
    return jax.shard_map(
        on_device,
        mesh=split,
        in_specs=placed,
        out_specs=(P("p", all_model, None), P("p", None, all_model), P()),
        check_vma=False,
    )
```
